32 devices in a mesh: dom: 8 (over z, y), sub: 4 (over x, core).
Axes of the slice: x: 2, y: 2, z: 4, core: 2. Of those that a mesh axis runs over, the one named last changes fastest.
Arguments:
- basis: float32 [2, 16, 32768], P(None, None, ('dom', 'sub')), may hold values from -6 to 6
- compact: float32 [2, 32, 16], replicated, may hold values from -1 to 1
- weights: float32 [2, 2, 32], replicated, may hold values from -5 to 5
- fresh: float32 [2, 32], replicated, may hold values from -1 to 1
- shifts: float32 [2, 2], replicated, may hold values from -1 to 1
- k_tiles: float32 [256, 3, 128, 128], P(('dom', 'sub'))
- pattern: int32 [256, 2], P(('dom', 'sub')), may hold values from 0 to 31
- mass: float32 [32768], P(('dom', 'sub')), may hold values from 0.5 to 2
- precond: float32 [256, 2, 128, 128], P(('dom', 'sub'))
- c_tiles: float32 [256, 128, 128], P(('dom', 'sub')), may hold values from -0.5 to 0.5
- c_rows: int32 [256], P(('dom', 'sub')), may hold values from 0 to 7
- c_side: int32 [256], P(('dom', 'sub')), may hold values from 0 to 1
- c_count: int32 [32], P(('dom', 'sub')), may hold values from 1 to 8, as said below
Outputs:
- new_basis: float32 [2, 2, 32768], P(None, None, ('dom', 'sub'))
- coeffs: float32 [2, 2, 18], replicated
The draws below stay inside these ranges and needn't reach their ends.
Inputs may be any that keep to these rules, and one draw needn't show every extreme that they name: `pattern`: each tile row's coupled tiles lie in its own domain group. `c_rows`: a tile row of the device itself. `c_side`: 0 reads the domain below, 1 the domain above. The live slots of device d are its first c_count[d]; some device has all 8 live.
All inputs are finite; a program needn't handle non-finite values.
Results may differ from the reference program's by a relative error of at most 0.0003.
Values sent between devices are 32-bit elements; how exact they have to be, the bound alone decides.
No kernel may reach another device: no remote copies, remote signals or barrier semaphores. Data moves between devices by JAX's collectives and lax.ppermute only.
A program may use at most 64 MiB of HBM per device.

```python
import math
import jax
import jax.numpy as jnp
from jax import lax

TILE = 128
TD = 8
NOFF = 2
CMAX = 8
NT = 32
NB = 16
ITERS = 3
STEPS = 2
TILES = 256
ROWS = 32768
SLOTS = 256
N_DOM = 8
N_SUB = 4
DEVICES = 32


def draw_k_tiles(key, part):
    shape = (TILES, NOFF + 1, TILE, TILE)
    noise = jax.random.normal(key, shape, jnp.float32)
    noise = noise / jnp.sqrt(jnp.float32(TILE))
    return noise.at[:, 0].add(5.0 * jnp.eye(TILE, dtype=jnp.float32))


def draw_precond(key, part):
    shape = (TILES, 2, TILE, TILE)
    noise = jax.random.normal(key, shape, jnp.float32)
    noise = 0.08 * noise / jnp.sqrt(jnp.float32(TILE))
    return noise.at[:, 0].add(0.2 * jnp.eye(TILE, dtype=jnp.float32))


def draw_c_count(key, part):
    first, second, third = jax.random.split(jax.random.fold_in(key, 11), 3)
    light = jax.random.randint(first, (DEVICES,), 1, CMAX // 4 + 2)
    heavy = jax.random.randint(second, (DEVICES,), 0, 8) == 0
    counts = jnp.where(heavy, CMAX, light)
    spot = jax.random.randint(third, (), 0, DEVICES)
    return counts.at[spot].set(CMAX).astype(jnp.int32)


def place_ends(entries, key, least, largest):
    shape = entries.shape
    spot = [jax.random.randint(jax.random.fold_in(key, axis), (), 0, shape[axis]) for axis in range(len(shape))]
    entries = entries.at[tuple(spot)].set(least)
    longest = shape.index(max(shape))
    spot[longest] = (spot[longest] + 1) % shape[longest]
    return entries.at[tuple(spot)].set(largest)


def levels(rng, extent, pieces, low, largest):
    gain, own = 1.0, jax.random.fold_in(rng, 6)
    for position, parts in pieces:
        steps = jnp.exp(jax.random.uniform(jax.random.fold_in(own, position), (parts,), jnp.float32, low / len(pieces), largest / len(pieces)))
        gain = gain * jnp.repeat(steps, extent[position] // parts).reshape([-1 if axis == position else 1 for axis in range(len(extent))])
    return gain


def bell_draw(rng, extent, width, bound, shards=(), kind=jnp.bfloat16):
    loudness = levels(rng, extent, shards, -0.22, 0.18) if shards else 1.0
    entries = jax.random.normal(rng, extent, jnp.float32) * width * loudness
    return jnp.minimum(jnp.maximum(entries, -bound), bound).astype(kind)


def setup_inputs(seed: int = 0) -> dict:
    arg_keys = jax.random.split(jax.random.key(seed), 14)
    basis = bell_draw(arg_keys[0], (2, NB, ROWS), 1.0, 6.0, ((2, 32),), jnp.float32)
    compact = bell_draw(arg_keys[1], (2, NT, NB), NT ** -0.5, 1.0, (), jnp.float32)
    weights = bell_draw(arg_keys[2], (STEPS, 2, NT), 1.0, 5.0, (), jnp.float32)
    fresh = bell_draw(arg_keys[3], (2, NT), NT ** -0.5, 1.0, (), jnp.float32)
    shifts = jnp.clip(jax.random.uniform(arg_keys[4], (STEPS, 2), jnp.float32, -1.0, 1.0), -1.0, 1.0)
    k_tiles = draw_k_tiles(jax.random.fold_in(arg_keys[13], 71), 0)
    pattern = place_ends(jax.random.randint(arg_keys[6], (TILES, NOFF), 0, TD * N_SUB), jax.random.fold_in(arg_keys[6], 1), 0, (TD * N_SUB) - 1).astype(jnp.int32)
    mass = jnp.clip(jnp.exp(math.log(2.0) - 1.3862944 * jax.random.uniform(arg_keys[7], (ROWS,), jnp.float32) ** levels(arg_keys[7], (ROWS,), ((0, 32),), -0.2, 0.2)), 0.5, 2.0)
    precond = draw_precond(jax.random.fold_in(arg_keys[13], 71), 0)
    c_tiles = bell_draw(arg_keys[9], (SLOTS, TILE, TILE), TILE ** -0.5, 0.5, ((0, 32),), jnp.float32)
    c_rows = place_ends(jax.random.randint(arg_keys[10], (SLOTS,), 0, TD), jax.random.fold_in(arg_keys[10], 1), 0, TD - 1).astype(jnp.int32)
    c_side = place_ends(jax.random.randint(arg_keys[11], (SLOTS,), 0, 2), jax.random.fold_in(arg_keys[11], 1), 0, 1).astype(jnp.int32)
    c_count = draw_c_count(jax.random.fold_in(arg_keys[13], 71), 0)
    return {"basis": basis, "compact": compact, "weights": weights, "fresh": fresh, "shifts": shifts, "k_tiles": k_tiles, "pattern": pattern, "mass": mass, "precond": precond, "c_tiles": c_tiles, "c_rows": c_rows, "c_side": c_side, "c_count": c_count}


HIGH = lax.Precision.HIGHEST
EPSILON = 1e-06

def solve_normal(matrix, vector):
    order = vector.shape[0]
    lower = [[None] * order for number in range(order)]
    for target in range(order):
        for source in range(target + 1):
            value = matrix[target, source]
            for middle in range(source):
                value = value - lower[target][middle] * lower[source][middle]
            if target == source:
                lower[target][target] = jnp.sqrt(value)
            else:
                lower[target][source] = value / lower[source][source]
    forward = []
    for target in range(order):
        value = vector[target]
        for middle in range(target):
            value = value - lower[target][middle] * forward[middle]
        forward.append(value / lower[target][target])
    result = [None] * order
    for target in reversed(range(order)):
        value = forward[target]
        for middle in range(target + 1, order):
            value = value - lower[middle][target] * result[middle]
        result[target] = value / lower[target][target]
    return jnp.stack(result)

def combine(coef_real, coef_imag, stack):
    real = jnp.dot(coef_real, stack[0], precision=HIGH) - jnp.dot(coef_imag, stack[1], precision=HIGH)
    imag = jnp.dot(coef_real, stack[1], precision=HIGH) + jnp.dot(coef_imag, stack[0], precision=HIGH)
    return jnp.stack([real, imag])

def conj_products(stack, vector):
    real = jnp.dot(stack[0], vector[0], precision=HIGH) + jnp.dot(stack[1], vector[1], precision=HIGH)
    imag = jnp.dot(stack[0], vector[1], precision=HIGH) - jnp.dot(stack[1], vector[0], precision=HIGH)
    return (real, imag)

def precondition(vector, precond):
    count, tile = (precond.shape[0], precond.shape[2])
    blocks = vector.reshape(2, count, tile)
    real = jnp.einsum('tij,tj->ti', precond[:, 0], blocks[0], precision=HIGH) - jnp.einsum('tij,tj->ti', precond[:, 1], blocks[1], precision=HIGH)
    imag = jnp.einsum('tij,tj->ti', precond[:, 0], blocks[1], precision=HIGH) + jnp.einsum('tij,tj->ti', precond[:, 1], blocks[0], precision=HIGH)
    return jnp.stack([real, imag]).reshape(2, -1)

def apply_shift(stiff, vector, mass, shift_pair):
    moved_real = mass * vector[0]
    moved_imag = mass * vector[1]
    real = stiff[0] - (shift_pair[0] * moved_real - shift_pair[1] * moved_imag)
    imag = stiff[1] - (shift_pair[0] * moved_imag + shift_pair[1] * moved_real)
    return jnp.stack([real, imag])

def gram_parts(stack):
    real = jnp.dot(stack[0], stack[0].T, precision=HIGH) + jnp.dot(stack[1], stack[1].T, precision=HIGH)
    imag = jnp.dot(stack[0], stack[1].T, precision=HIGH) - jnp.dot(stack[1], stack[0].T, precision=HIGH)
    return (real, imag)

def minimal_coefficients(gram_real, gram_imag, order):
    top = jnp.concatenate([gram_real[:order, :order], -gram_imag[:order, :order]], axis=1)
    bottom = jnp.concatenate([gram_imag[:order, :order], gram_real[:order, :order]], axis=1)
    system = jnp.concatenate([top, bottom], axis=0)
    target = jnp.concatenate([gram_real[:order, order], gram_imag[:order, order]])
    solved = solve_normal(system, target)
    return (solved[:order], solved[order:])

def operate(vector, shift_pair, k_tiles, pattern, mass, c_tiles, c_rows, c_side, c_count):
    tiles_total = k_tiles.shape[0]
    tile = k_tiles.shape[2]
    group = TD * N_SUB
    blocks = vector.reshape(2, tiles_total, tile)
    ownrow = jnp.arange(tiles_total, dtype=jnp.int32)
    columns = jnp.concatenate([ownrow[:, None], (ownrow // group * group)[:, None] + pattern], axis=1)
    picked = blocks[:, columns]
    stiff = jnp.einsum('tsij,ctsj->cti', k_tiles, picked, precision=HIGH).reshape(2, -1)
    result = apply_shift(stiff, vector, mass, shift_pair)
    slots = jnp.arange(c_tiles.shape[0], dtype=jnp.int32)
    device = slots // CMAX
    within = slots % CMAX
    domain = device // N_SUB
    source_tile = jnp.where(c_side == 0, (device - N_SUB) * TD + TD - 1, (device + N_SUB) * TD)
    present = jnp.where(c_side == 0, domain > 0, domain < N_DOM - 1)
    valid = ((within < c_count[device]) & present).astype(jnp.float32)
    source_tile = jnp.clip(source_tile, 0, tiles_total - 1).astype(jnp.int32)
    contrib = jnp.einsum('sij,csj->csi', c_tiles, blocks[:, source_tile], precision=HIGH) * valid[None, :, None]
    landing = (device * TD + c_rows).astype(jnp.int32)
    extra = jnp.zeros((2, tiles_total, tile), jnp.float32).at[:, landing].add(contrib)
    return result + extra.reshape(2, -1)

def reference(basis, compact, weights, fresh, shifts, k_tiles, pattern, mass, precond, c_tiles, c_rows, c_side, c_count):
    total_rows = basis.shape[2]
    previous = jnp.zeros((2, total_rows), jnp.float32)
    made = []
    listed = []
    for step in range(STEPS):
        beta_real = weights[step, 0]
        beta_imag = weights[step, 1]
        coef_real = jnp.dot(beta_real, compact[0], precision=HIGH) - jnp.dot(beta_imag, compact[1], precision=HIGH)
        coef_imag = jnp.dot(beta_real, compact[1], precision=HIGH) + jnp.dot(beta_imag, compact[0], precision=HIGH)
        gamma_real = jnp.sum(beta_real * fresh[0] - beta_imag * fresh[1])
        gamma_imag = jnp.sum(beta_real * fresh[1] + beta_imag * fresh[0])
        extended = jnp.concatenate([basis, previous[:, None, :]], axis=1)
        right = combine(jnp.concatenate([coef_real, gamma_real[None]]), jnp.concatenate([coef_imag, gamma_imag[None]]), extended)
        terms = [right]
        images = []
        for index in range(ITERS):
            image = operate(precondition(terms[-1], precond), shifts[step], k_tiles, pattern, mass, c_tiles, c_rows, c_side, c_count)
            images.append(image)
            if index + 1 < ITERS:
                terms.append(image - terms[-1])
        stacked = jnp.stack(images + [right], axis=1)
        gram_real, gram_imag = gram_parts(stacked)
        solve_real, solve_imag = minimal_coefficients(gram_real, gram_imag, ITERS)
        direction = combine(solve_real, solve_imag, jnp.stack(terms, axis=1))
        solution = precondition(direction, precond)
        proj_real, proj_imag = conj_products(extended, solution)
        proj_real = proj_real / ROWS
        proj_imag = proj_imag / ROWS
        remain = solution - combine(proj_real, proj_imag, extended)
        norm = jnp.sqrt(jnp.sum(remain * remain) / ROWS + EPSILON)
        latest = remain / norm
        made.append(latest)
        listed.append(jnp.stack([jnp.concatenate([proj_real, norm[None]]), jnp.concatenate([proj_imag, jnp.zeros((1,), jnp.float32)])]))
        previous = latest
    return (jnp.stack(made), jnp.stack(listed))
```

```python
import functools
import jax
import jax.numpy as jnp
from jax import lax
from jax.experimental import pallas as pl
from jax.experimental.pallas import tpu as pltpu
from jax.sharding import PartitionSpec as P

ITERS = 3
EPSILON = 1e-06
HIGH = lax.Precision.HIGHEST
F32 = jnp.float32
BF16 = jnp.bfloat16
NT_DIMS = (((1,), (1,)), ((), ()))
LANES = 128
AXES = ("dom", "sub")


def iota(shape, dim):
    return lax.broadcasted_iota(jnp.int32, shape, dim)


def split(x):
    high = x.astype(BF16).astype(F32)
    return high, x - high


def cmul(a, b):
    return a[0] * b[0] - a[1] * b[1], a[0] * b[1] + a[1] * b[0]


def conj(a):
    return a[0], -a[1]


def csub(a, b):
    return a[0] - b[0], a[1] - b[1]


def cadd(a, b):
    return a[0] + b[0], a[1] + b[1]


def scale(a, s):
    return a[0] * s, a[1] * s


def nt_dot(a, b, precision=None):
    return lax.dot_general(a, b, NT_DIMS, precision=precision, preferred_element_type=F32)


def store_parts(high_ref, low_ref, block, x):
    lanes = slice(block * LANES, (block + 1) * LANES)
    high, low = split(x)
    high_ref[:, lanes] = high.astype(BF16)
    low_ref[:, lanes] = low.astype(BF16)


def product(high_ref, low_ref, wide_ref, blocks):
    lanes = blocks * LANES
    wide = wide_ref[:, :lanes]
    total = nt_dot(high_ref[...], wide) + nt_dot(low_ref[...], wide)
    flipped = total.T
    rows = flipped.shape[0] // 4
    parts = [flipped[k * rows : (k + 1) * rows] for k in range(4)]
    return parts[0] + parts[2], parts[1] + parts[3]


def put(wide_ref, block, parts):
    wide_ref[:, block * LANES : (block + 1) * LANES] = jnp.concatenate(parts, axis=0).astype(BF16)


def parts_of(vector):
    real, imag = vector
    real_high, real_low = split(real)
    imag_high, imag_low = split(imag)
    return [real_high, imag_high, real_low, imag_low]


def precondition(vector, high_ref, low_ref, wide_ref):
    tiles = vector[0].shape[0]
    straight = parts_of(vector)
    turned = [-straight[1], straight[0], -straight[3], straight[2]]
    row = iota(vector[0].shape, 0)
    for tile in range(tiles):
        mask = row == tile
        put(wide_ref, 2 * tile, [jnp.where(mask, x, 0.0) for x in straight])
        put(wide_ref, 2 * tile + 1, [jnp.where(mask, x, 0.0) for x in turned])
    return product(high_ref, low_ref, wide_ref, 2 * tiles)


def load(ref):
    rows = ref.shape[0] // 2
    return ref[:rows], ref[rows:]


def save(ref, vector):
    ref[...] = jnp.concatenate(vector, axis=0)


def send(vector, first_ref, second_ref):
    even = lax.rem(lax.axis_index("dom"), 2) == 0
    rows = vector[0].shape[0]
    head = jnp.concatenate([vector[0][:1], vector[1][:1]], axis=0)
    tail = jnp.concatenate([vector[0][rows - 1 :], vector[1][rows - 1 :]], axis=0)
    first_ref[...] = jnp.where(even, tail, head)
    second_ref[...] = jnp.where(even, head, tail)


def mix_basis(coef, basis_ref):
    real, imag = coef
    tiles = basis_ref.shape[2] // LANES
    row = iota((tiles, LANES), 0)
    out_real = jnp.zeros((tiles, LANES), F32)
    out_imag = jnp.zeros((tiles, LANES), F32)
    for tile in range(tiles):
        lanes = slice(tile * LANES, (tile + 1) * LANES)
        base_real, base_imag = basis_ref[0, :, lanes], basis_ref[1, :, lanes]
        sum_real = jnp.sum(real * base_real - imag * base_imag, axis=0, keepdims=True)
        sum_imag = jnp.sum(real * base_imag + imag * base_real, axis=0, keepdims=True)
        out_real = jnp.where(row == tile, sum_real, out_real)
        out_imag = jnp.where(row == tile, sum_imag, out_imag)
    return out_real, out_imag


def coefficients(step, compact_ref, weights_ref, fresh_ref):
    beta = weights_ref[step]
    part_real = lax.dot_general(
        beta, compact_ref[0], (((1,), (0,)), ((), ())), precision=HIGH, preferred_element_type=F32
    )
    part_imag = lax.dot_general(
        beta, compact_ref[1], (((1,), (0,)), ((), ())), precision=HIGH, preferred_element_type=F32
    )
    row_real = part_real[0:1] - part_imag[1:2]
    row_imag = part_imag[0:1] + part_real[1:2]
    count = compact_ref.shape[2]
    same = iota((count, count), 0) == iota((count, count), 1)
    coef_real = jnp.sum(jnp.where(same, row_real, 0.0), axis=1, keepdims=True)
    coef_imag = jnp.sum(jnp.where(same, row_imag, 0.0), axis=1, keepdims=True)
    fresh = fresh_ref[...]
    gamma_real = jnp.sum(beta[0:1] * fresh[0:1] - beta[1:2] * fresh[1:2], axis=1, keepdims=True)
    gamma_imag = jnp.sum(beta[0:1] * fresh[1:2] + beta[1:2] * fresh[0:1], axis=1, keepdims=True)
    return (coef_real, coef_imag), (gamma_real, gamma_imag)


def start_kernel(
    basis_ref, compact_ref, weights_ref, fresh_ref, precond_ref,
    right_ref, image_ref, first_ref, second_ref, high_ref, low_ref,
    wide_ref,
):
    for tile in range(precond_ref.shape[0]):
        for part in range(2):
            store_parts(high_ref, low_ref, 2 * tile + part, precond_ref[tile, part])
    coef, _ = coefficients(0, compact_ref, weights_ref, fresh_ref)
    right = mix_basis(coef, basis_ref)
    save(right_ref, right)
    image = precondition(right, high_ref, low_ref, wide_ref)
    save(image_ref, image)
    send(image, first_ref, second_ref)


def prepare_kernel(
    n_dom, pattern_ref, rows_ref, side_ref, count_ref, basis_ref, k_ref, c_ref,
    high_ref, low_ref, pick_ref, below_ref, above_ref, inner_ref,
):
    tiles, slots_k = k_ref.shape[0], k_ref.shape[1]
    for tile in range(tiles):
        for slot in range(slots_k):
            store_parts(high_ref, low_ref, tile * slots_k + slot, k_ref[tile, slot])
    slots = c_ref.shape[0]
    for slot in range(slots):
        store_parts(high_ref, low_ref, tiles * slots_k + slot, c_ref[slot])
    mine = lax.axis_index("sub") * tiles
    row, lane = iota(pick_ref.shape, 0), iota(pick_ref.shape, 1)
    picked = jnp.zeros(pick_ref.shape, F32)
    for slot in range(slots_k - 1):
        for tile in range(tiles):
            column = pattern_ref[tile, slot] ^ mine
            picked = jnp.where((row == slot * tiles + tile) & (lane == column), 1.0, picked)
    pick_ref[...] = picked.astype(BF16)
    domain = lax.axis_index("dom")
    row = iota((tiles, LANES), 0)
    for slot in range(slots):
        live = slot < count_ref[0]
        side = side_ref[slot]
        here = row == rows_ref[slot]
        low_on = live & (side == 0) & (domain > 0)
        high_on = live & (side != 0) & (domain < n_dom - 1)
        below_ref[slot] = jnp.where(here & low_on, 1.0, 0.0)
        above_ref[slot] = jnp.where(here & high_on, 1.0, 0.0)
    real, imag = basis_ref[0], basis_ref[1]
    inner = nt_dot(real, jnp.concatenate([real, imag], axis=0), HIGH)
    inner = inner + nt_dot(imag, jnp.concatenate([imag, -real], axis=0), HIGH)
    inner_ref[...] = jnp.zeros(inner_ref.shape, F32)
    half, wide = inner_ref.shape[0], inner.shape[1]
    inner_ref[:, 6 * half : 6 * half + wide] = inner[:half]
    inner_ref[:, 6 * half + wide : 6 * half + 2 * wide] = inner[half:]


def operate(
    step, image_ref, blocks, first_ref, second_ref, shifts_ref, mass_ref,
    high_ref, low_ref, pick_ref, below_ref, above_ref, wide_ref,
):
    image = load(image_ref)
    tiles = image[0].shape[0]
    own = parts_of(image)
    gathered = [own] + [parts_of(load(block)) for block in blocks]
    table = jnp.concatenate(
        [jnp.concatenate([g[part] for g in gathered], axis=0) for part in range(4)], axis=1
    ).astype(BF16)
    chosen = jnp.dot(pick_ref[...], table, preferred_element_type=F32)
    others = chosen.shape[0] // tiles
    row = iota(image[0].shape, 0)
    for tile in range(tiles):
        mask = row == tile
        base = tile * (others + 1)
        put(wide_ref, base, [jnp.where(mask, x, 0.0) for x in own])
        for slot in range(others):
            rows = slice(slot * tiles, (slot + 1) * tiles)
            put(
                wide_ref,
                base + 1 + slot,
                [
                    jnp.where(mask, chosen[rows, part * LANES : (part + 1) * LANES], 0.0)
                    for part in range(4)
                ],
            )
    even = lax.rem(lax.axis_index("dom"), 2) == 0
    first, second = first_ref[...], second_ref[...]
    below = jnp.where(even, second, first)
    above = jnp.where(even, first, second)
    below = parts_of((below[0:1], below[1:2]))
    above = parts_of((above[0:1], above[1:2]))
    slots = below_ref.shape[0]
    base = tiles * (others + 1)
    for slot in range(slots):
        low_mask, high_mask = below_ref[slot], above_ref[slot]
        put(
            wide_ref,
            base + slot,
            [low_mask * below[part] + high_mask * above[part] for part in range(4)],
        )
    stiff = product(high_ref, low_ref, wide_ref, base + slots)
    mass = mass_ref[...]
    moved = (mass * image[0], mass * image[1])
    shift_real, shift_imag = shifts_ref[step, 0], shifts_ref[step, 1]
    real = stiff[0] - (shift_real * moved[0] - shift_imag * moved[1])
    imag = stiff[1] - (shift_real * moved[1] + shift_imag * moved[0])
    return real, imag


def level_kernel(step, others, image_ref, term_ref, *refs):
    blocks, refs = refs[:others], refs[others:]
    (
        first_in, second_in, shifts_ref, mass_ref, k_high, k_low, pick_ref, below_ref, above_ref,
        p_high, p_low, result_ref, next_ref, out_ref, first_ref, second_ref, wide_ref,
    ) = refs
    result = operate(
        step, image_ref, blocks, first_in, second_in, shifts_ref, mass_ref,
        k_high, k_low, pick_ref, below_ref, above_ref, wide_ref,
    )
    save(result_ref, result)
    term = csub(result, load(term_ref))
    save(next_ref, term)
    image = precondition(term, p_high, p_low, wide_ref)
    save(out_ref, image)
    send(image, first_ref, second_ref)


def last_kernel(step, others, image_ref, term_ref, *refs):
    blocks, refs = refs[:others], refs[others:]
    (
        first_in, second_in, shifts_ref, mass_ref, k_high, k_low, pick_ref, below_ref, above_ref,
        basis_ref, previous_ref, inner_ref,
    ) = refs[:12]
    earlier, refs = refs[12 : 12 + 2 * ITERS - 1], refs[12 + 2 * ITERS - 1 :]
    payload_ref, wide_ref, rows_ref = refs
    result = operate(
        step, image_ref, blocks, first_in, second_in, shifts_ref, mass_ref,
        k_high, k_low, pick_ref, below_ref, above_ref, wide_ref,
    )
    results = [load(ref) for ref in earlier[: ITERS - 1]] + [result]
    right = load(earlier[ITERS - 1])
    images = [load(ref) for ref in earlier[ITERS:]] + [load(image_ref)]
    vectors = results + [right] + images + [load(previous_ref)]
    count = len(vectors)
    for index, (real, imag) in enumerate(vectors):
        rows_ref[:, index, :] = real
        rows_ref[:, count + index, :] = imag
        rows_ref[:, 2 * count + index, :] = imag
        rows_ref[:, 3 * count + index, :] = -real
    tiles = rows_ref.shape[0]
    lefts, rights = [], []
    for tile in range(tiles):
        lanes = slice(tile * LANES, (tile + 1) * LANES)
        for part in range(2):
            left = rows_ref[tile, part * count : (part + 1) * count]
            lefts.append(jnp.concatenate([basis_ref[part, :, lanes], left], axis=0))
            rights.append(rows_ref[tile, 2 * part * count : 2 * (part + 1) * count])
    left = jnp.concatenate(lefts, axis=1)
    right_rows = jnp.concatenate(rights, axis=1)
    right_rows = jnp.concatenate([right_rows] * 3, axis=0)
    table = nt_dot(left, right_rows, HIGH)
    width = 2 * count
    lane = iota((count, 3 * width), 1)
    merged = jnp.where(
        lane < width, table[:count], jnp.where(lane < 2 * width, table[count : 2 * count], table[2 * count :])
    )
    total = jnp.concatenate(
        [merged, inner_ref[:, 3 * width :]], axis=1
    )

    @pl.loop(0, payload_ref.shape[0])
    def _(device):
        payload_ref[device] = total


def settle(
    total_rows, sums, inner, basis_ref, images, previous,
):
    count = sums.shape[0]
    width = 2 * count
    shape = sums.shape

    def column(lane, table=sums):
        return jnp.broadcast_to(table[:, lane : lane + 1], shape)

    def cell(row, lane):
        return jnp.broadcast_to(column(lane)[row : row + 1], shape)

    def entry(row, col):
        base = 2 * width
        return cell(row, base + col), cell(row, base + count + col)

    gram = {(a, b): entry(a, b) for a in range(ITERS) for b in range(a, ITERS)}
    target = [entry(a, ITERS) for a in range(ITERS)]
    lower, pivots = {}, []
    for col in range(ITERS):
        pivot = gram[col, col][0]
        for mid in range(col):
            real, imag = lower[col, mid]
            pivot = pivot - (real * real + imag * imag) * pivots[mid]
        pivots.append(pivot)
        for row in range(col + 1, ITERS):
            value = conj(gram[col, row])
            for mid in range(col):
                value = csub(value, scale(cmul(lower[row, mid], conj(lower[col, mid])), pivots[mid]))
            lower[row, col] = (value[0] / pivot, value[1] / pivot)
    forward = []
    for row in range(ITERS):
        value = target[row]
        for mid in range(row):
            value = csub(value, cmul(lower[row, mid], forward[mid]))
        forward.append(value)
    solved = [None] * ITERS
    for row in reversed(range(ITERS)):
        value = (forward[row][0] / pivots[row], forward[row][1] / pivots[row])
        for mid in range(row + 1, ITERS):
            value = csub(value, cmul(conj(lower[mid, row]), solved[mid]))
        solved[row] = value

    offset = ITERS + 1
    square = jnp.zeros(shape, F32)
    for a in range(ITERS):
        square = square + (solved[a][0] ** 2 + solved[a][1] ** 2) * entry(offset + a, offset + a)[0]
        for b in range(a + 1, ITERS):
            pair = cmul(conj(solved[a]), solved[b])
            square = square + 2.0 * cmul(pair, entry(offset + a, offset + b))[0]

    projections = []
    for block in range(2):
        base = block * width
        value = None
        for a in range(ITERS):
            term = cmul(solved[a], (column(base + offset + a), column(base + count + offset + a)))
            value = term if value is None else cadd(value, term)
        projections.append(scale(value, 1.0 / total_rows))
    value = None
    for a in range(ITERS):
        term = cmul(solved[a], entry(count - 1, offset + a))
        value = term if value is None else cadd(value, term)
    extra = scale(value, 1.0 / total_rows)

    row, lane = iota(shape, 0), iota(shape, 1)
    first = 3 * width
    span = 4 * count
    first_row = jnp.zeros(shape, F32)
    second_row = jnp.zeros(shape, F32)
    for block in range(2):
        real, imag = projections[block]
        at_real = (lane == first + block * count + row) | (lane == first + span + block * count + row)
        at_imag = (lane == first + 2 * count + block * count + row) | (
            lane == first + span + 2 * count + block * count + row
        )
        first_row = first_row + jnp.where(at_real, real, jnp.where(at_imag, -imag, 0.0))
        second_row = second_row + jnp.where(at_real, imag, jnp.where(at_imag, real, 0.0))
    first_row = jnp.sum(first_row, axis=0, keepdims=True)
    second_row = jnp.sum(second_row, axis=0, keepdims=True)
    upper = lane < first + span
    real_col = jnp.where(upper, projections[0][0], projections[1][0])
    imag_col = jnp.where(upper, projections[0][1], projections[1][1])
    quad = jnp.sum(inner * (real_col * first_row + imag_col * second_row), axis=1, keepdims=True)
    quad = jnp.broadcast_to(quad, shape)
    for block in range(2):
        base = block * width
        real, imag = projections[block]
        cross = cmul(
            cmul((real, -imag), extra), (column(base + count - 1), column(base + width - 1))
        )[0]
        quad = quad + 2.0 * cross - 2.0 * total_rows * (real * real + imag * imag)
    quad = jnp.broadcast_to(jnp.sum(quad, axis=0, keepdims=True), shape)
    extra_size = extra[0] * extra[0] + extra[1] * extra[1]
    quad = quad + extra_size * (entry(count - 1, count - 1)[0] - 2.0 * total_rows)
    norm = jnp.sqrt((square + quad) * (1.0 / total_rows) + EPSILON)

    coef = tuple(
        jnp.concatenate([projections[0][part], projections[1][part]], axis=0) for part in range(2)
    )
    mixed = cadd(mix_basis(coef, basis_ref), cmul(extra, previous))
    made = None
    for a in range(ITERS):
        term = cmul(solved[a], images[a])
        made = term if made is None else cadd(made, term)
    remain = csub(made, mixed)
    latest = (remain[0] / norm, remain[1] / norm)

    rows = []
    for part in range(2):
        spread = jnp.zeros(shape, F32)
        for block in range(2):
            spread = spread + jnp.where(lane == block * count + row, projections[block][part], 0.0)
        spread = jnp.sum(spread, axis=0, keepdims=True)
        spread = spread + jnp.where(lane[:1] == 2 * count, extra[part][:1], 0.0)
        if part == 0:
            spread = spread + jnp.where(lane[:1] == 2 * count + 1, norm[:1], 0.0)
        rows.append(spread)
    return latest, jnp.concatenate(rows, axis=0)


def reduce_sums(sums_ref):
    if sums_ref.shape[0] <= 64:
        values = [sums_ref[k] for k in range(sums_ref.shape[0])]
        while len(values) > 1:
            values = [
                values[k] + values[k + 1] if k + 1 < len(values) else values[k]
                for k in range(0, len(values), 2)
            ]
        return values[0]
    return jnp.sum(sums_ref[...], axis=0)


def between_kernel(
    total_rows, step, sums_ref, basis_ref, compact_ref, weights_ref, fresh_ref, p_high, p_low,
    *refs,
):
    images = [load(ref) for ref in refs[:ITERS]]
    previous_ref = refs[ITERS]
    (right_ref, image_ref, first_ref, second_ref, latest_ref, coeffs_ref, inner_ref, wide_ref) = refs[
        ITERS + 1 :
    ]
    sums = reduce_sums(sums_ref)
    inner_ref[...] = sums
    latest, coeffs = settle(total_rows, sums, sums, basis_ref, images, load(previous_ref))
    save(latest_ref, latest)
    coeffs_ref[...] = coeffs
    coef, gamma = coefficients(step + 1, compact_ref, weights_ref, fresh_ref)
    right = cadd(mix_basis(coef, basis_ref), cmul(gamma, latest))
    save(right_ref, right)
    image = precondition(right, p_high, p_low, wide_ref)
    save(image_ref, image)
    send(image, first_ref, second_ref)


def finish_kernel(total_rows, sums_ref, inner_ref, basis_ref, *refs):
    images = [load(ref) for ref in refs[:ITERS]]
    previous_ref, before_ref, made_ref, listed_ref = refs[ITERS:]
    sums = reduce_sums(sums_ref)
    previous = load(previous_ref)
    latest, coeffs = settle(total_rows, sums, inner_ref[...], basis_ref, images, previous)
    for step, vector in enumerate((previous, latest)):
        for part in range(2):
            for tile in range(vector[part].shape[0]):
                made_ref[step, part : part + 1, tile * LANES : (tile + 1) * LANES] = vector[part][
                    tile : tile + 1
                ]
    width = listed_ref.shape[2]
    listed_ref[0] = before_ref[:, :width]
    listed_ref[1] = coeffs[:, :width]


def vmem():
    return pl.BlockSpec(memory_space=pltpu.VMEM)


def smem():
    return pl.BlockSpec(memory_space=pltpu.SMEM)


def call(kernel, name, out_shape, in_specs, scratch, args, flops=10**7):
    return pl.pallas_call(
        kernel,
        name=name,
        out_shape=out_shape,
        in_specs=in_specs,
        out_specs=jax.tree.map(lambda _: vmem(), out_shape),
        scratch_shapes=scratch,
        cost_estimate=pl.CostEstimate(flops=flops, bytes_accessed=10**6, transcendentals=0),
    )(*args)


def local(
    n_dom,
    n_sub,
    basis,
    compact,
    weights,
    fresh,
    shifts,
    k_tiles,
    pattern,
    mass,
    precond,
    c_tiles,
    c_rows,
    c_side,
    c_count,
):
    tiles, slots_k, tile = k_tiles.shape[0], k_tiles.shape[1], k_tiles.shape[2]
    slots = c_tiles.shape[0]
    devices = n_dom * n_sub
    total_rows = float(tiles * tile * devices)
    steps = weights.shape[0]
    vec = jax.ShapeDtypeStruct((2 * tiles, tile), F32)
    edge = jax.ShapeDtypeStruct((2, tile), F32)
    square = jax.ShapeDtypeStruct((tiles, tile), F32)
    k_blocks = tiles * slots_k + slots
    p_blocks = 2 * tiles
    k_part = jax.ShapeDtypeStruct((tile, k_blocks * tile), BF16)
    p_part = jax.ShapeDtypeStruct((tile, p_blocks * tile), BF16)
    mask = jax.ShapeDtypeStruct((slots, tiles, tile), F32)
    pick = jax.ShapeDtypeStruct(((slots_k - 1) * tiles, tiles * n_sub), BF16)
    wide = pltpu.VMEM((4 * tiles, max(k_blocks, p_blocks) * tile), BF16)
    mass = mass.reshape(tiles, tile)
    zero = jnp.zeros((2 * tiles, tile), F32)

    even_swap = [(i, i ^ 1) for i in range(n_dom)]
    odd_swap = [(i, (i + 1 if i % 2 else i - 1) % n_dom) for i in range(n_dom)]

    def exchange(image, first, second):
        second = lax.ppermute(second, "dom", odd_swap)
        first = lax.ppermute(first, "dom", even_swap)
        blocks = [
            lax.ppermute(image, "sub", [(i, i ^ k) for i in range(n_sub)]) for k in range(1, n_sub)
        ]
        return blocks, first, second

    right, image, first, second, p_high, p_low = call(
        start_kernel, "start", (vec, vec, edge, edge, p_part, p_part), [vmem()] * 5, [wide],
        (basis, compact, weights, fresh, precond),
    )
    k_high, k_low, pick_table, below, above, inner = call(
        functools.partial(prepare_kernel, n_dom), "prepare",
        (k_part, k_part, pick, mask, mask, square), [smem()] * 4 + [vmem()] * 3, [],
        (pattern, c_rows, c_side, c_count, basis, k_tiles, c_tiles),
    )
    others = n_sub - 1
    previous = zero
    for step in range(steps):
        term = right
        images, results = [image], []
        for index in range(ITERS):
            blocks, first_in, second_in = exchange(images[-1], first, second)
            common = (
                images[-1], term, *blocks, first_in, second_in, shifts, mass, k_high, k_low,
                pick_table, below, above,
            )
            specs = [vmem()] * (4 + others) + [smem()] + [vmem()] * 6
            if index + 1 < ITERS:
                result, term, image, first, second = call(
                    functools.partial(level_kernel, step, others), "level",
                    (vec, vec, vec, edge, edge), specs + [vmem()] * 2, [wide],
                    common + (p_high, p_low),
                )
                results.append(result)
                images.append(image)
            else:
                earlier = (*results, right, *images[:-1])
                payload = call(
                    functools.partial(last_kernel, step, others), "last",
                    jax.ShapeDtypeStruct((devices, tiles, tile), F32),
                    specs + [vmem()] * (3 + len(earlier)),
                    [wide, pltpu.VMEM((tiles, 4 * (2 * ITERS + 2), tile), F32)],
                    common + (basis, previous, inner, *earlier),
                )
        sums = lax.all_to_all(payload, AXES, 0, 0)
        if step + 1 < steps:
            right, image, first, second, previous_next, coeffs, inner_sum = call(
                functools.partial(between_kernel, total_rows, step), "between",
                (vec, vec, edge, edge, vec, jax.ShapeDtypeStruct((2, tile), F32), square),
                [vmem()] * (8 + ITERS), [wide],
                (sums, basis, compact, weights, fresh, p_high, p_low, *images, previous),
            )
            previous = previous_next
        else:
            width = basis.shape[1] + 2
            made, listed = call(
                functools.partial(finish_kernel, total_rows), "finish",
                (
                    jax.ShapeDtypeStruct((steps, 2, tiles * tile), F32),
                    jax.ShapeDtypeStruct((steps, 2, width), F32),
                ),
                [vmem()] * (5 + ITERS), [],
                (sums, inner_sum, basis, *images, previous, coeffs),
            )
    return made, listed


def solution(mesh):
    placed = (
        P(None, None, AXES),
        P(),
        P(),
        P(),
        P(),
        P(AXES, None, None, None),
        P(AXES, None),
        P(AXES),
        P(AXES, None, None, None),
        P(AXES, None, None),
        P(AXES),
        P(AXES),
        P(AXES),
    )
    return jax.shard_map(
        functools.partial(local, mesh.shape["dom"], mesh.shape["sub"]),
        mesh=mesh,
        in_specs=placed,
        out_specs=(P(None, None, AXES), P()),
        check_vma=False,
    )
```

```python
import functools
import jax
import jax.numpy as jnp
from jax import lax
from jax.experimental import pallas as pl
from jax.experimental.pallas import tpu as pltpu
from jax.sharding import PartitionSpec as P

ITERS = 3
EPSILON = 1e-06
HIGH = lax.Precision.HIGHEST
F32 = jnp.float32
BF16 = jnp.bfloat16
NT_DIMS = (((1,), (1,)), ((), ()))
LANES = 128
VMEM_LIMIT = 12 * 1024 * 1024
AXES = ("dom", "sub")


def iota(shape, dim):
    return lax.broadcasted_iota(jnp.int32, shape, dim)


def split(x):
    high = x.astype(BF16).astype(F32)
    return high, x - high


def cmul(a, b):
    return a[0] * b[0] - a[1] * b[1], a[0] * b[1] + a[1] * b[0]


def conj(a):
    return a[0], -a[1]


def csub(a, b):
    return a[0] - b[0], a[1] - b[1]


def cadd(a, b):
    return a[0] + b[0], a[1] + b[1]


def scale(a, s):
    return a[0] * s, a[1] * s


def nt_dot(a, b, precision=None):
    return lax.dot_general(a, b, NT_DIMS, precision=precision, preferred_element_type=F32)


def store_parts(high_ref, low_ref, block, x):
    lanes = slice(block * LANES, (block + 1) * LANES)
    high, low = split(x)
    high_ref[:, lanes] = high.astype(BF16)
    low_ref[:, lanes] = low.astype(BF16)


def product(high_ref, low_ref, wide_ref, blocks):
    lanes = blocks * LANES
    wide = wide_ref[:, :lanes]
    total = nt_dot(high_ref[...], wide) + nt_dot(low_ref[...], wide)
    flipped = total.T
    rows = flipped.shape[0] // 4
    parts = [flipped[k * rows : (k + 1) * rows] for k in range(4)]
    return parts[0] + parts[2], parts[1] + parts[3]


def put(wide_ref, block, parts):
    wide_ref[:, block * LANES : (block + 1) * LANES] = jnp.concatenate(parts, axis=0).astype(BF16)


def parts_of(vector):
    real, imag = vector
    real_high, real_low = split(real)
    imag_high, imag_low = split(imag)
    return [real_high, imag_high, real_low, imag_low]


def precondition(vector, high_ref, low_ref, wide_ref):
    tiles = vector[0].shape[0]
    straight = parts_of(vector)
    turned = [-straight[1], straight[0], -straight[3], straight[2]]
    row = iota(vector[0].shape, 0)
    for tile in range(tiles):
        mask = row == tile
        put(wide_ref, 2 * tile, [jnp.where(mask, x, 0.0) for x in straight])
        put(wide_ref, 2 * tile + 1, [jnp.where(mask, x, 0.0) for x in turned])
    return product(high_ref, low_ref, wide_ref, 2 * tiles)


def load(ref):
    rows = ref.shape[0] // 2
    return ref[:rows], ref[rows:]


def save(ref, vector):
    ref[...] = jnp.concatenate(vector, axis=0)


def send(vector, first_ref, second_ref):
    even = lax.rem(lax.axis_index("dom"), 2) == 0
    rows = vector[0].shape[0]
    head = jnp.concatenate([vector[0][:1], vector[1][:1]], axis=0)
    tail = jnp.concatenate([vector[0][rows - 1 :], vector[1][rows - 1 :]], axis=0)
    first_ref[...] = jnp.where(even, tail, head)
    second_ref[...] = jnp.where(even, head, tail)


def mix_basis(coef, basis_ref):
    real, imag = coef
    tiles = basis_ref.shape[2] // LANES
    row = iota((tiles, LANES), 0)
    out_real = jnp.zeros((tiles, LANES), F32)
    out_imag = jnp.zeros((tiles, LANES), F32)
    for tile in range(tiles):
        lanes = slice(tile * LANES, (tile + 1) * LANES)
        base_real, base_imag = basis_ref[0, :, lanes], basis_ref[1, :, lanes]
        sum_real = jnp.sum(real * base_real - imag * base_imag, axis=0, keepdims=True)
        sum_imag = jnp.sum(real * base_imag + imag * base_real, axis=0, keepdims=True)
        out_real = jnp.where(row == tile, sum_real, out_real)
        out_imag = jnp.where(row == tile, sum_imag, out_imag)
    return out_real, out_imag


def coefficients(step, compact_ref, weights_ref, fresh_ref):
    beta = weights_ref[step]
    beta_real, beta_imag = beta[0:1], beta[1:2]
    compact_real, compact_imag = compact_ref[0], compact_ref[1]
    coef_real = jnp.sum(compact_real * beta_real - compact_imag * beta_imag, axis=1, keepdims=True)
    coef_imag = jnp.sum(compact_imag * beta_real + compact_real * beta_imag, axis=1, keepdims=True)
    fresh = fresh_ref[...]
    gamma_real = jnp.sum(beta_real * fresh[0:1] - beta_imag * fresh[1:2], axis=1, keepdims=True)
    gamma_imag = jnp.sum(beta_real * fresh[1:2] + beta_imag * fresh[0:1], axis=1, keepdims=True)
    return (coef_real, coef_imag), (gamma_real, gamma_imag)


def start_kernel(
    basis_in, compact_in, weights_in, fresh_in, precond_in,
    right_ref, image_ref, first_ref, second_ref, high_ref, low_ref,
    basis_ref, compact_ref, weights_ref, fresh_ref,
    wide_ref, precond_ref, small_sem, tile_sem,
):
    moves = [
        pltpu.make_async_copy(source, target, small_sem.at[index])
        for index, (source, target) in enumerate(
            (
                (compact_in, compact_ref),
                (weights_in, weights_ref),
                (fresh_in, fresh_ref),
                (basis_in, basis_ref),
            )
        )
    ]
    for move in moves:
        move.start()
    tiles = precond_in.shape[0]
    tile_moves = [
        pltpu.make_async_copy(precond_in.at[tile], precond_ref.at[tile], tile_sem.at[tile])
        for tile in range(tiles)
    ]
    for move in tile_moves:
        move.start()
    for move in moves:
        move.wait()
    coef, _ = coefficients(0, compact_ref, weights_ref, fresh_ref)
    right = mix_basis(coef, basis_ref)
    save(right_ref, right)
    for tile in range(tiles):
        tile_moves[tile].wait()
        for part in range(2):
            store_parts(high_ref, low_ref, 2 * tile + part, precond_ref[tile, part])
    image = precondition(right, high_ref, low_ref, wide_ref)
    save(image_ref, image)
    send(image, first_ref, second_ref)


def prepare_kernel(
    n_dom, pattern_in, rows_in, side_in, count_ref, shifts_in, mass_in, k_in, c_in, basis_ref,
    high_ref, low_ref, c_high_ref, c_low_ref, pick_ref, below_ref, above_ref, inner_ref, drag_ref,
    k_ref, c_ref, mass_ref, pattern_ref, rows_ref, side_ref, shifts_ref,
    small_sem, k_sem,
):
    moves = [
        pltpu.make_async_copy(source, target, small_sem.at[index])
        for index, (source, target) in enumerate(
            (
                (pattern_in, pattern_ref),
                (rows_in, rows_ref),
                (side_in, side_ref),
                (shifts_in, shifts_ref),
                (mass_in, mass_ref),
                (c_in, c_ref),
            )
        )
    ]
    for move in moves:
        move.start()
    tiles, slots_k = k_in.shape[0], k_in.shape[1]
    k_moves = [
        pltpu.make_async_copy(k_in.at[tile], k_ref.at[tile], k_sem.at[tile]) for tile in range(tiles)
    ]
    for move in k_moves:
        move.start()
    real, imag = basis_ref[0], basis_ref[1]
    inner = nt_dot(real, jnp.concatenate([real, imag], axis=0), HIGH)
    inner = inner + nt_dot(imag, jnp.concatenate([imag, -real], axis=0), HIGH)
    inner_ref[...] = jnp.zeros(inner_ref.shape, F32)
    half, wide = inner_ref.shape[0], inner.shape[1]
    inner_ref[:, 6 * half : 6 * half + wide] = inner[:half]
    inner_ref[:, 6 * half + wide : 6 * half + 2 * wide] = inner[half:]
    for move in moves:
        move.wait()
    mine = lax.axis_index("sub") * tiles
    row, lane = iota(pick_ref.shape, 0), iota(pick_ref.shape, 1)
    picked = jnp.zeros(pick_ref.shape, F32)
    for slot in range(slots_k - 1):
        for tile in range(tiles):
            column = pattern_ref[slot, tile] ^ mine
            picked = jnp.where((row == slot * tiles + tile) & (lane == column), 1.0, picked)
    pick_ref[...] = picked.astype(BF16)
    domain = lax.axis_index("dom")
    row = iota((tiles, LANES), 0)
    slots = c_ref.shape[0]
    for slot in range(slots):
        live = slot < count_ref[0]
        side = side_ref[slot]
        here = row == rows_ref[slot]
        low_on = live & (side == 0) & (domain > 0)
        high_on = live & (side != 0) & (domain < n_dom - 1)
        below_ref[slot] = jnp.where(here & low_on, 1.0, 0.0)
        above_ref[slot] = jnp.where(here & high_on, 1.0, 0.0)
    mass = mass_ref[...]
    for step in range(drag_ref.shape[0]):
        for part in range(2):
            drag_ref[step, part] = mass * shifts_ref[step, part]
    for slot in range(slots):
        store_parts(c_high_ref, c_low_ref, slot, c_ref[slot])
    for tile in range(tiles):
        k_moves[tile].wait()
        for slot in range(slots_k):
            store_parts(high_ref, low_ref, tile * slots_k + slot, k_ref[tile, slot])


def stiff_kernel(step, image_ref, *refs):
    blocks, (drag_ref, high_ref, low_ref, pick_ref, result_ref, wide_ref) = refs[:-6], refs[-6:]
    image = load(image_ref)
    tiles = image[0].shape[0]
    own = parts_of(image)
    gathered = [own] + [parts_of(load(block)) for block in blocks]
    table = jnp.concatenate(
        [jnp.concatenate([g[part] for g in gathered], axis=0) for part in range(4)], axis=1
    ).astype(BF16)
    chosen = jnp.dot(pick_ref[...], table, preferred_element_type=F32)
    others = chosen.shape[0] // tiles
    row = iota(image[0].shape, 0)
    for tile in range(tiles):
        mask = row == tile
        base = tile * (others + 1)
        put(wide_ref, base, [jnp.where(mask, x, 0.0) for x in own])
        for slot in range(others):
            rows = slice(slot * tiles, (slot + 1) * tiles)
            put(
                wide_ref,
                base + 1 + slot,
                [
                    jnp.where(mask, chosen[rows, part * LANES : (part + 1) * LANES], 0.0)
                    for part in range(4)
                ],
            )
    stiff = product(high_ref, low_ref, wide_ref, tiles * (others + 1))
    drag = cmul((drag_ref[step, 0], drag_ref[step, 1]), image)
    save(result_ref, csub(stiff, drag))


def couple(partial_ref, first_ref, second_ref, high_ref, low_ref, below_ref, above_ref, wide_ref):
    even = lax.rem(lax.axis_index("dom"), 2) == 0
    first, second = first_ref[...], second_ref[...]
    below = jnp.where(even, second, first)
    above = jnp.where(even, first, second)
    below = parts_of((below[0:1], below[1:2]))
    above = parts_of((above[0:1], above[1:2]))
    slots = below_ref.shape[0]
    for slot in range(slots):
        low_mask, high_mask = below_ref[slot], above_ref[slot]
        put(wide_ref, slot, [low_mask * below[part] + high_mask * above[part] for part in range(4)])
    return cadd(load(partial_ref), product(high_ref, low_ref, wide_ref, slots))


def level_kernel(
    partial_ref, first_in, second_in, c_high, c_low, below_ref, above_ref, term_ref, p_high, p_low,
    result_ref, next_ref, out_ref, first_ref, second_ref, wide_ref,
):
    result = couple(
        partial_ref, first_in, second_in, c_high, c_low, below_ref, above_ref, wide_ref
    )
    save(result_ref, result)
    term = csub(result, load(term_ref))
    save(next_ref, term)
    image = precondition(term, p_high, p_low, wide_ref)
    save(out_ref, image)
    send(image, first_ref, second_ref)


def gram_kernel(basis_ref, previous_ref, inner_ref, *refs):
    refs, (out_ref, rows_ref) = refs[:-2], refs[-2:]
    results = [load(ref) for ref in refs[: ITERS - 1]]
    right = load(refs[ITERS - 1])
    images = [load(ref) for ref in refs[ITERS:]]
    zero = jnp.zeros(right[0].shape, F32)
    vectors = results + [(zero, zero), right] + images + [load(previous_ref)]
    count = len(vectors)
    for index, (real, imag) in enumerate(vectors):
        rows_ref[:, index, :] = real
        rows_ref[:, count + index, :] = imag
        rows_ref[:, 2 * count + index, :] = imag
        rows_ref[:, 3 * count + index, :] = -real
    tiles = rows_ref.shape[0]
    lefts, rights = [], []
    for tile in range(tiles):
        lanes = slice(tile * LANES, (tile + 1) * LANES)
        for part in range(2):
            left = rows_ref[tile, part * count : (part + 1) * count]
            lefts.append(jnp.concatenate([basis_ref[part, :, lanes], left], axis=0))
            rights.append(rows_ref[tile, 2 * part * count : 2 * (part + 1) * count])
    left = jnp.concatenate(lefts, axis=1)
    right_rows = jnp.concatenate(rights, axis=1)
    right_rows = jnp.concatenate([right_rows] * 3, axis=0)
    table = nt_dot(left, right_rows, HIGH)
    width = 2 * count
    lane = iota((count, 3 * width), 1)
    merged = jnp.where(
        lane < width,
        table[:count],
        jnp.where(lane < 2 * width, table[count : 2 * count], table[2 * count :]),
    )
    out_ref[...] = jnp.concatenate([merged, inner_ref[:, 3 * width :]], axis=1)


def last_kernel(
    partial_ref, first_in, second_in, c_high, c_low, below_ref, above_ref, sums_ref, *refs
):
    earlier, (payload_ref, wide_ref) = refs[:-2], refs[-2:]
    result = couple(
        partial_ref, first_in, second_in, c_high, c_low, below_ref, above_ref, wide_ref
    )
    vectors = [load(ref) for ref in earlier[: ITERS - 1]]
    total = sums_ref[...]
    count = total.shape[0]
    row, lane = iota(total.shape, 0), iota(total.shape, 1)
    base = 4 * count
    last = ITERS - 1
    pairs = [(index, last, vector, result) for index, vector in enumerate(vectors)]
    pairs += [(last, last, result, result), (last, ITERS, result, load(earlier[last]))]
    for at_row, at_col, left, right in pairs:
        real = left[0] * right[0] + left[1] * right[1]
        imag = left[0] * right[1] - left[1] * right[0]
        for part, value in enumerate((real, imag)):
            value = jnp.sum(jnp.sum(value, axis=0, keepdims=True), axis=1, keepdims=True)
            spot = (row == at_row) & (lane == base + part * count + at_col)
            total = jnp.where(spot, value, total)

    @pl.loop(0, payload_ref.shape[0])
    def _(device):
        payload_ref[device] = total


def settle(
    total_rows, sums, inner, basis_ref, images, previous,
):
    count = sums.shape[0]
    width = 2 * count
    shape = sums.shape

    def column(lane, table=sums):
        return jnp.broadcast_to(table[:, lane : lane + 1], shape)

    def cell(row, lane):
        return jnp.broadcast_to(column(lane)[row : row + 1], shape)

    def entry(row, col):
        base = 2 * width
        return cell(row, base + col), cell(row, base + count + col)

    gram = {(a, b): entry(a, b) for a in range(ITERS) for b in range(a, ITERS)}
    target = [entry(a, ITERS) for a in range(ITERS)]
    lower, pivots = {}, []
    for col in range(ITERS):
        pivot = gram[col, col][0]
        for mid in range(col):
            real, imag = lower[col, mid]
            pivot = pivot - (real * real + imag * imag) * pivots[mid]
        pivots.append(pivot)
        for row in range(col + 1, ITERS):
            value = conj(gram[col, row])
            for mid in range(col):
                value = csub(value, scale(cmul(lower[row, mid], conj(lower[col, mid])), pivots[mid]))
            lower[row, col] = (value[0] / pivot, value[1] / pivot)
    forward = []
    for row in range(ITERS):
        value = target[row]
        for mid in range(row):
            value = csub(value, cmul(lower[row, mid], forward[mid]))
        forward.append(value)
    solved = [None] * ITERS
    for row in reversed(range(ITERS)):
        value = (forward[row][0] / pivots[row], forward[row][1] / pivots[row])
        for mid in range(row + 1, ITERS):
            value = csub(value, cmul(conj(lower[mid, row]), solved[mid]))
        solved[row] = value

    offset = ITERS + 1
    square = jnp.zeros(shape, F32)
    for a in range(ITERS):
        square = square + (solved[a][0] ** 2 + solved[a][1] ** 2) * entry(offset + a, offset + a)[0]
        for b in range(a + 1, ITERS):
            pair = cmul(conj(solved[a]), solved[b])
            square = square + 2.0 * cmul(pair, entry(offset + a, offset + b))[0]

    projections = []
    for block in range(2):
        base = block * width
        value = None
        for a in range(ITERS):
            term = cmul(solved[a], (column(base + offset + a), column(base + count + offset + a)))
            value = term if value is None else cadd(value, term)
        projections.append(scale(value, 1.0 / total_rows))
    value = None
    for a in range(ITERS):
        term = cmul(solved[a], entry(count - 1, offset + a))
        value = term if value is None else cadd(value, term)
    extra = scale(value, 1.0 / total_rows)

    row, lane = iota(shape, 0), iota(shape, 1)
    first = 3 * width
    span = 4 * count
    first_row = jnp.zeros(shape, F32)
    second_row = jnp.zeros(shape, F32)
    for block in range(2):
        real, imag = projections[block]
        at_real = (lane == first + block * count + row) | (lane == first + span + block * count + row)
        at_imag = (lane == first + 2 * count + block * count + row) | (
            lane == first + span + 2 * count + block * count + row
        )
        first_row = first_row + jnp.where(at_real, real, jnp.where(at_imag, -imag, 0.0))
        second_row = second_row + jnp.where(at_real, imag, jnp.where(at_imag, real, 0.0))
    first_row = jnp.sum(first_row, axis=0, keepdims=True)
    second_row = jnp.sum(second_row, axis=0, keepdims=True)
    upper = lane < first + span
    real_col = jnp.where(upper, projections[0][0], projections[1][0])
    imag_col = jnp.where(upper, projections[0][1], projections[1][1])
    quad = jnp.sum(inner * (real_col * first_row + imag_col * second_row), axis=1, keepdims=True)
    quad = jnp.broadcast_to(quad, shape)
    for block in range(2):
        base = block * width
        real, imag = projections[block]
        cross = cmul(
            cmul((real, -imag), extra), (column(base + count - 1), column(base + width - 1))
        )[0]
        quad = quad + 2.0 * cross - 2.0 * total_rows * (real * real + imag * imag)
    quad = jnp.broadcast_to(jnp.sum(quad, axis=0, keepdims=True), shape)
    extra_size = extra[0] * extra[0] + extra[1] * extra[1]
    quad = quad + extra_size * (entry(count - 1, count - 1)[0] - 2.0 * total_rows)
    norm = jnp.sqrt((square + quad) * (1.0 / total_rows) + EPSILON)

    coef = tuple(
        jnp.concatenate([projections[0][part], projections[1][part]], axis=0) for part in range(2)
    )
    mixed = cadd(mix_basis(coef, basis_ref), cmul(extra, previous))
    made = None
    for a in range(ITERS):
        term = cmul(solved[a], images[a])
        made = term if made is None else cadd(made, term)
    remain = csub(made, mixed)
    latest = (remain[0] / norm, remain[1] / norm)

    rows = []
    for part in range(2):
        spread = jnp.zeros(shape, F32)
        for block in range(2):
            spread = spread + jnp.where(lane == block * count + row, projections[block][part], 0.0)
        spread = jnp.sum(spread, axis=0, keepdims=True)
        spread = spread + jnp.where(lane[:1] == 2 * count, extra[part][:1], 0.0)
        if part == 0:
            spread = spread + jnp.where(lane[:1] == 2 * count + 1, norm[:1], 0.0)
        rows.append(spread)
    return latest, jnp.concatenate(rows, axis=0)


def reduce_sums(sums_ref):
    if sums_ref.shape[0] <= 64:
        values = [sums_ref[k] for k in range(sums_ref.shape[0])]
        while len(values) > 1:
            values = [
                values[k] + values[k + 1] if k + 1 < len(values) else values[k]
                for k in range(0, len(values), 2)
            ]
        return values[0]
    return jnp.sum(sums_ref[...], axis=0)


def between_kernel(
    total_rows, step, sums_ref, basis_ref, compact_ref, weights_ref, fresh_ref, p_high, p_low,
    *refs,
):
    images = [load(ref) for ref in refs[:ITERS]]
    previous_ref = refs[ITERS]
    (right_ref, image_ref, first_ref, second_ref, latest_ref, coeffs_ref, inner_ref, wide_ref) = refs[
        ITERS + 1 :
    ]
    sums = reduce_sums(sums_ref)
    inner_ref[...] = sums
    latest, coeffs = settle(total_rows, sums, sums, basis_ref, images, load(previous_ref))
    save(latest_ref, latest)
    coeffs_ref[...] = coeffs
    coef, gamma = coefficients(step + 1, compact_ref, weights_ref, fresh_ref)
    right = cadd(mix_basis(coef, basis_ref), cmul(gamma, latest))
    save(right_ref, right)
    image = precondition(right, p_high, p_low, wide_ref)
    save(image_ref, image)
    send(image, first_ref, second_ref)


def finish_kernel(total_rows, sums_ref, inner_ref, basis_ref, *refs):
    images = [load(ref) for ref in refs[:ITERS]]
    previous_ref, before_ref, made_ref, listed_ref = refs[ITERS:]
    sums = reduce_sums(sums_ref)
    previous = load(previous_ref)
    latest, coeffs = settle(total_rows, sums, inner_ref[...], basis_ref, images, previous)
    for step, vector in enumerate((previous, latest)):
        for part in range(2):
            for tile in range(vector[part].shape[0]):
                made_ref[step, part : part + 1, tile * LANES : (tile + 1) * LANES] = vector[part][
                    tile : tile + 1
                ]
    width = listed_ref.shape[2]
    listed_ref[0] = before_ref[:, :width]
    listed_ref[1] = coeffs[:, :width]


def vmem():
    return pl.BlockSpec(memory_space=pltpu.VMEM)


def hbm():
    return pl.BlockSpec(memory_space=pltpu.HBM)


def smem():
    return pl.BlockSpec(memory_space=pltpu.SMEM)


def in_hbm(*arrays):
    return tuple(pltpu.with_memory_space_constraint(array, pltpu.HBM) for array in arrays)


def shape_of(array):
    return jax.ShapeDtypeStruct(array.shape, array.dtype)


def call(kernel, out_shape, in_specs, scratch, args, flops=10**7):
    return pl.pallas_call(
        kernel,
        out_shape=out_shape,
        in_specs=in_specs,
        out_specs=jax.tree.map(lambda _: vmem(), out_shape),
        scratch_shapes=scratch,
        cost_estimate=pl.CostEstimate(flops=flops, bytes_accessed=10**6, transcendentals=0),
        compiler_params=pltpu.CompilerParams(vmem_limit_bytes=VMEM_LIMIT),
    )(*args)


def local(
    n_dom,
    n_sub,
    basis,
    compact,
    weights,
    fresh,
    shifts,
    k_tiles,
    pattern,
    mass,
    precond,
    c_tiles,
    c_rows,
    c_side,
    c_count,
):
    tiles, slots_k, tile = k_tiles.shape[0], k_tiles.shape[1], k_tiles.shape[2]
    slots = c_tiles.shape[0]
    devices = n_dom * n_sub
    total_rows = float(tiles * tile * devices)
    steps = weights.shape[0]
    vec = jax.ShapeDtypeStruct((2 * tiles, tile), F32)
    edge = jax.ShapeDtypeStruct((2, tile), F32)
    square = jax.ShapeDtypeStruct((tiles, tile), F32)
    k_blocks = tiles * slots_k
    p_blocks = 2 * tiles
    k_part = jax.ShapeDtypeStruct((tile, k_blocks * tile), BF16)
    c_part = jax.ShapeDtypeStruct((tile, slots * tile), BF16)
    p_part = jax.ShapeDtypeStruct((tile, p_blocks * tile), BF16)
    mask = jax.ShapeDtypeStruct((slots, tiles, tile), F32)
    pick = jax.ShapeDtypeStruct(((slots_k - 1) * tiles, tiles * n_sub), BF16)
    drag = jax.ShapeDtypeStruct((steps, 2, tiles, tile), F32)
    compact = jnp.swapaxes(compact, 1, 2)
    pattern = pattern.T
    mass = mass.reshape(tiles, tile)
    zero = jnp.zeros((2 * tiles, tile), F32)

    def wide(blocks):
        return pltpu.VMEM((4 * tiles, blocks * tile), BF16)

    even_swap = [(i, i ^ 1) for i in range(n_dom)]
    odd_swap = [(i, (i + 1 if i % 2 else i - 1) % n_dom) for i in range(n_dom)]

    def exchange(image, first, second):
        second = lax.ppermute(second, "dom", odd_swap)
        first = lax.ppermute(first, "dom", even_swap)
        blocks = []
        for k in range(1, n_sub):
            blocks.append(lax.ppermute(image, "sub", [(i, i ^ k) for i in range(n_sub)]))
        return blocks, first, second

    right, image, first, second, p_high, p_low, basis, compact, weights, fresh = call(
        start_kernel,
        (vec, vec, edge, edge, p_part, p_part, shape_of(basis), shape_of(compact), shape_of(weights), shape_of(fresh)),
        [hbm()] * 5,
        [
            wide(p_blocks),
            pltpu.VMEM(precond.shape, F32),
            pltpu.SemaphoreType.DMA((4,)),
            pltpu.SemaphoreType.DMA((tiles,)),
        ],
        in_hbm(basis, compact, weights, fresh, precond),
    )
    k_high, k_low, c_high, c_low, pick_table, below, above, inner, drag = call(
        functools.partial(prepare_kernel, n_dom),
        (k_part, k_part, c_part, c_part, pick, mask, mask, square, drag),
        [hbm()] * 3 + [smem()] + [hbm()] * 4 + [vmem()],
        [
            pltpu.VMEM(k_tiles.shape, F32),
            pltpu.VMEM(c_tiles.shape, F32),
            pltpu.VMEM(mass.shape, F32),
            pltpu.SMEM(pattern.shape, jnp.int32),
            pltpu.SMEM(c_rows.shape, jnp.int32),
            pltpu.SMEM(c_side.shape, jnp.int32),
            pltpu.SMEM(shifts.shape, F32),
            pltpu.SemaphoreType.DMA((6,)),
            pltpu.SemaphoreType.DMA((tiles,)),
        ],
        in_hbm(pattern, c_rows, c_side)
        + (c_count,)
        + in_hbm(shifts, mass, k_tiles, c_tiles)
        + (basis,),
    )
    previous = zero
    for step in range(steps):
        term = right
        images, results = [image], []
        for index in range(ITERS):
            blocks, first_in, second_in = exchange(image, first, second)
            partial = call(
                functools.partial(stiff_kernel, step), vec, [vmem()] * (n_sub + 4),
                [wide(k_blocks)], (image, *blocks, drag, k_high, k_low, pick_table),
            )
            common = (partial, first_in, second_in, c_high, c_low, below, above)
            if index + 1 < ITERS:
                result, term, image, first, second = call(
                    level_kernel, (vec, vec, vec, edge, edge), [vmem()] * 10,
                    [wide(max(slots, p_blocks))], common + (term, p_high, p_low),
                )
                results.append(result)
                images.append(image)
            else:
                sums = call(
                    gram_kernel, square, [vmem()] * (3 + 2 * ITERS),
                    [pltpu.VMEM((tiles, 4 * tiles, tile), F32)],
                    (basis, previous, inner, *results, right, *images),
                )
                payload = call(
                    last_kernel, jax.ShapeDtypeStruct((devices, tiles, tile), F32),
                    [vmem()] * (8 + ITERS), [wide(slots)], common + (sums, *results, right),
                )
        sums = lax.all_to_all(payload, AXES, 0, 0)
        if step + 1 < steps:
            right, image, first, second, latest, coeffs, inner_sum = call(
                functools.partial(between_kernel, total_rows, step),
                (vec, vec, edge, edge, vec, jax.ShapeDtypeStruct((2, tile), F32), square),
                [vmem()] * (8 + ITERS), [wide(p_blocks)],
                (sums, basis, compact, weights, fresh, p_high, p_low, *images, previous),
            )
            previous = latest
        else:
            width = basis.shape[1] + 2
            made, listed = call(
                functools.partial(finish_kernel, total_rows),
                (
                    jax.ShapeDtypeStruct((steps, 2, tiles * tile), F32),
                    jax.ShapeDtypeStruct((steps, 2, width), F32),
                ),
                [vmem()] * (5 + ITERS), [],
                (sums, inner_sum, basis, *images, previous, coeffs),
            )
    return made, listed


def solution(mesh):
    placed = (
        P(None, None, AXES),
        P(),
        P(),
        P(),
        P(),
        P(AXES, None, None, None),
        P(AXES, None),
        P(AXES),
        P(AXES, None, None, None),
        P(AXES, None, None),
        P(AXES),
        P(AXES),
        P(AXES),
    )
    return jax.shard_map(
        functools.partial(local, mesh.shape["dom"], mesh.shape["sub"]),
        mesh=mesh,
        in_specs=placed,
        out_specs=(P(None, None, AXES), P()),
        check_vma=False,
    )
```

```python
import functools
import jax
import jax.numpy as jnp
from jax import lax
from jax.experimental import pallas as pl
from jax.experimental.pallas import tpu as pltpu
from jax.sharding import PartitionSpec as P

ITERS = 3
EPSILON = 1e-06
HIGH = lax.Precision.HIGHEST
F32 = jnp.float32
BF16 = jnp.bfloat16
NT_DIMS = (((1,), (1,)), ((), ()))
LANES = 128
COPIED = 11
FOLD = 4
VMEM_LIMIT = 12 * 1024 * 1024
AXES = ("dom", "sub")


def iota(shape, dim):
    return lax.broadcasted_iota(jnp.int32, shape, dim)


def split(x):
    high = x.astype(BF16).astype(F32)
    return high, x - high


def cmul(a, b):
    return a[0] * b[0] - a[1] * b[1], a[0] * b[1] + a[1] * b[0]


def conj(a):
    return a[0], -a[1]


def csub(a, b):
    return a[0] - b[0], a[1] - b[1]


def cadd(a, b):
    return a[0] + b[0], a[1] + b[1]


def scale(a, s):
    return a[0] * s, a[1] * s


def nt_dot(a, b, precision=None):
    return lax.dot_general(a, b, NT_DIMS, precision=precision, preferred_element_type=F32)


def store_parts(high_ref, low_ref, block, x):
    lanes = slice(block * LANES, (block + 1) * LANES)
    high, low = split(x)
    high_ref[:, lanes] = high.astype(BF16)
    low_ref[:, lanes] = low.astype(BF16)


def product(high_ref, low_ref, wide_ref, blocks):
    lanes = blocks * LANES
    wide = wide_ref[:, :lanes]
    total = nt_dot(high_ref[...], wide) + nt_dot(low_ref[...], wide)
    flipped = total.T
    rows = flipped.shape[0] // 4
    parts = [flipped[k * rows : (k + 1) * rows] for k in range(4)]
    return parts[0] + parts[2], parts[1] + parts[3]


def put(wide_ref, block, parts):
    wide_ref[:, block * LANES : (block + 1) * LANES] = jnp.concatenate(parts, axis=0).astype(BF16)


def parts_of(vector):
    real, imag = vector
    real_high, real_low = split(real)
    imag_high, imag_low = split(imag)
    return [real_high, imag_high, real_low, imag_low]


def precondition(vector, high_ref, low_ref, wide_ref):
    tiles = vector[0].shape[0]
    straight = parts_of(vector)
    turned = [-straight[1], straight[0], -straight[3], straight[2]]
    row = iota(vector[0].shape, 0)
    for tile in range(tiles):
        mask = row == tile
        put(wide_ref, 2 * tile, [jnp.where(mask, x, 0.0) for x in straight])
        put(wide_ref, 2 * tile + 1, [jnp.where(mask, x, 0.0) for x in turned])
    return product(high_ref, low_ref, wide_ref, 2 * tiles)


def load(ref):
    rows = ref.shape[0] // 2
    return ref[:rows], ref[rows:]


def save(ref, vector):
    ref[...] = jnp.concatenate(vector, axis=0)


def send(vector, first_ref, second_ref):
    even = lax.rem(lax.axis_index("dom"), 2) == 0
    rows = vector[0].shape[0]
    head = jnp.concatenate([vector[0][:1], vector[1][:1]], axis=0)
    tail = jnp.concatenate([vector[0][rows - 1 :], vector[1][rows - 1 :]], axis=0)
    first_ref[...] = jnp.where(even, tail, head)
    second_ref[...] = jnp.where(even, head, tail)


def mix_basis(coef, basis_ref):
    real, imag = coef
    tiles = basis_ref.shape[2] // LANES
    row = iota((tiles, LANES), 0)
    out_real = jnp.zeros((tiles, LANES), F32)
    out_imag = jnp.zeros((tiles, LANES), F32)
    for tile in range(tiles):
        lanes = slice(tile * LANES, (tile + 1) * LANES)
        base_real, base_imag = basis_ref[0, :, lanes], basis_ref[1, :, lanes]
        sum_real = jnp.sum(real * base_real - imag * base_imag, axis=0, keepdims=True)
        sum_imag = jnp.sum(real * base_imag + imag * base_real, axis=0, keepdims=True)
        out_real = jnp.where(row == tile, sum_real, out_real)
        out_imag = jnp.where(row == tile, sum_imag, out_imag)
    return out_real, out_imag


def coefficients(step, compact_ref, weights_ref, fresh_ref):
    beta = weights_ref[step]
    beta_real, beta_imag = beta[0:1], beta[1:2]
    compact_real, compact_imag = compact_ref[0], compact_ref[1]
    coef_real = jnp.sum(compact_real * beta_real - compact_imag * beta_imag, axis=1, keepdims=True)
    coef_imag = jnp.sum(compact_imag * beta_real + compact_real * beta_imag, axis=1, keepdims=True)
    fresh = fresh_ref[...]
    gamma_real = jnp.sum(beta_real * fresh[0:1] - beta_imag * fresh[1:2], axis=1, keepdims=True)
    gamma_imag = jnp.sum(beta_real * fresh[1:2] + beta_imag * fresh[0:1], axis=1, keepdims=True)
    return (coef_real, coef_imag), (gamma_real, gamma_imag)


def start_kernel(*refs):
    sources, refs = refs[:COPIED], refs[COPIED:]
    precond_in, refs = refs[0], refs[1:]
    right_ref, image_ref, first_ref, second_ref, high_ref, low_ref = refs[:6]
    targets, refs = refs[6 : 6 + COPIED], refs[6 + COPIED :]
    wide_ref, precond_ref, small_sem, tile_sem = refs
    moves = [
        pltpu.make_async_copy(source, target, small_sem.at[index])
        for index, (source, target) in enumerate(zip(sources, targets))
    ]
    tiles = precond_in.shape[0]
    tile_moves = [
        pltpu.make_async_copy(precond_in.at[tile], precond_ref.at[tile], tile_sem.at[tile])
        for tile in range(tiles)
    ]
    early, late = moves[:4], moves[4:]
    for move in early + tile_moves + late:
        move.start()
    for move in early:
        move.wait()
    basis_ref, compact_ref, weights_ref, fresh_ref = targets[:4]
    coef, _ = coefficients(0, compact_ref, weights_ref, fresh_ref)
    right = mix_basis(coef, basis_ref)
    save(right_ref, right)
    for tile in range(tiles):
        tile_moves[tile].wait()
        for part in range(2):
            store_parts(high_ref, low_ref, 2 * tile + part, precond_ref[tile, part])
    image = precondition(right, high_ref, low_ref, wide_ref)
    save(image_ref, image)
    send(image, first_ref, second_ref)
    for move in late:
        move.wait()


def as_column(row):
    count = row.shape[1]
    same = iota((count, count), 0) == iota((count, count), 1)
    return jnp.sum(jnp.where(same, row, 0.0), axis=1, keepdims=True)


def prepare_kernel(
    n_dom, count_ref, pattern_ref, rows_ref, side_ref, shifts_ref, mass_ref, k_ref, c_ref,
    high_ref, low_ref, c_high_ref, c_low_ref, pick_ref, below_ref, above_ref, drag_ref,
):
    tiles, slots_k, slots = k_ref.shape[0], k_ref.shape[1], c_ref.shape[0]
    for tile in range(tiles):
        for slot in range(slots_k):
            store_parts(high_ref, low_ref, tile * slots_k + slot, k_ref[tile, slot])
    for slot in range(slots):
        store_parts(c_high_ref, c_low_ref, slot, c_ref[slot])
    mine = lax.axis_index("sub") * tiles
    lane = iota((tiles, pick_ref.shape[1]), 1) ^ mine
    lane = lane.astype(F32)
    picked = [
        jnp.where(as_column(pattern_ref[slot : slot + 1].astype(F32)) == lane, 1.0, 0.0)
        for slot in range(slots_k - 1)
    ]
    pick_ref[...] = jnp.concatenate(picked, axis=0).astype(BF16)
    domain = lax.axis_index("dom")
    shape = (tiles, LANES)
    row = iota(shape, 0)
    for slot in range(slots):
        live = slot < count_ref[0]
        side = jnp.broadcast_to(side_ref[:, slot : slot + 1], shape)
        here = row == jnp.broadcast_to(rows_ref[:, slot : slot + 1], shape)
        low_on = jnp.where(live & (domain > 0), 1.0, 0.0)
        high_on = jnp.where(live & (domain < n_dom - 1), 1.0, 0.0)
        below_ref[slot] = jnp.where(here & (side == 0), low_on, 0.0)
        above_ref[slot] = jnp.where(here & (side != 0), high_on, 0.0)
    mass = mass_ref[...]
    for step in range(drag_ref.shape[0]):
        for part in range(2):
            shift = jnp.broadcast_to(shifts_ref[step : step + 1, part : part + 1], shape)
            drag_ref[step, part] = mass * shift


def inner_kernel(basis_ref, after_ref, inner_ref):
    real, imag = basis_ref[0], basis_ref[1]
    inner = nt_dot(real, jnp.concatenate([real, imag], axis=0), HIGH)
    inner = inner + nt_dot(imag, jnp.concatenate([imag, -real], axis=0), HIGH)
    inner_ref[...] = jnp.zeros(inner_ref.shape, F32)
    half, wide = inner_ref.shape[0], inner.shape[1]
    inner_ref[:, 4 * half : 4 * half + wide] = inner[:half]
    inner_ref[:, 4 * half + wide : 4 * half + 2 * wide] = inner[half:]


def stiff_kernel(step, others, image_ref, *refs):
    blocks, (drag_ref, high_ref, low_ref, pick_ref) = refs[:others], refs[others : others + 4]
    result_ref, wide_ref = refs[-2:]
    image = load(image_ref)
    tiles = image[0].shape[0]
    own = parts_of(image)
    gathered = [own] + [parts_of(load(block)) for block in blocks]
    table = jnp.concatenate(
        [jnp.concatenate([g[part] for g in gathered], axis=0) for part in range(4)], axis=1
    ).astype(BF16)
    chosen = jnp.dot(pick_ref[...], table, preferred_element_type=F32)
    others = chosen.shape[0] // tiles
    row = iota(image[0].shape, 0)
    for tile in range(tiles):
        mask = row == tile
        base = tile * (others + 1)
        put(wide_ref, base, [jnp.where(mask, x, 0.0) for x in own])
        for slot in range(others):
            rows = slice(slot * tiles, (slot + 1) * tiles)
            put(
                wide_ref,
                base + 1 + slot,
                [
                    jnp.where(mask, chosen[rows, part * LANES : (part + 1) * LANES], 0.0)
                    for part in range(4)
                ],
            )
    stiff = product(high_ref, low_ref, wide_ref, tiles * (others + 1))
    drag = cmul((drag_ref[step, 0], drag_ref[step, 1]), image)
    save(result_ref, csub(stiff, drag))


def couple(partial_ref, first_ref, second_ref, high_ref, low_ref, below_ref, above_ref, wide_ref):
    even = lax.rem(lax.axis_index("dom"), 2) == 0
    first, second = first_ref[...], second_ref[...]
    below = jnp.where(even, second, first)
    above = jnp.where(even, first, second)
    below = parts_of((below[0:1], below[1:2]))
    above = parts_of((above[0:1], above[1:2]))
    slots = below_ref.shape[0]
    for slot in range(slots):
        low_mask, high_mask = below_ref[slot], above_ref[slot]
        put(wide_ref, slot, [low_mask * below[part] + high_mask * above[part] for part in range(4)])
    return cadd(load(partial_ref), product(high_ref, low_ref, wide_ref, slots))


def level_kernel(
    partial_ref, first_in, second_in, c_high, c_low, below_ref, above_ref, term_ref, p_high, p_low,
    result_ref, out_ref, first_ref, second_ref, *refs,
):
    next_refs, wide_ref = refs[:-1], refs[-1]
    result = couple(
        partial_ref, first_in, second_in, c_high, c_low, below_ref, above_ref, wide_ref
    )
    save(result_ref, result)
    term = csub(result, load(term_ref))
    for next_ref in next_refs:
        save(next_ref, term)
    image = precondition(term, p_high, p_low, wide_ref)
    save(out_ref, image)
    send(image, first_ref, second_ref)


def gram_kernel(basis_ref, previous_ref, inner_ref, *refs):
    refs, (out_ref, rows_ref) = refs[:-2], refs[-2:]
    results = [load(ref) for ref in refs[: ITERS - 1]]
    right = load(refs[ITERS - 1])
    images = [load(ref) for ref in refs[ITERS:]]
    zero = jnp.zeros(right[0].shape, F32)
    vectors = results + [(zero, zero), right] + images + [load(previous_ref)]
    count = len(vectors)
    for index, (real, imag) in enumerate(vectors):
        rows_ref[:, index, :] = real
        rows_ref[:, count + index, :] = imag
        rows_ref[:, 2 * count + index, :] = imag
        rows_ref[:, 3 * count + index, :] = -real
    tiles = rows_ref.shape[0]
    lefts, rights, chosen = [], [], []
    half = count // 2
    for tile in range(tiles):
        lanes = slice(tile * LANES, (tile + 1) * LANES)
        for part in range(2):
            left = rows_ref[tile, part * count : (part + 1) * count]
            lefts.append(jnp.concatenate([basis_ref[part, :, lanes], left], axis=0))
            base = 2 * part * count
            rights.append(rows_ref[tile, base : base + 2 * count])
            chosen.append(
                jnp.concatenate(
                    [
                        rows_ref[tile, base + half : base + count],
                        rows_ref[tile, base + count + half : base + 2 * count],
                    ],
                    axis=0,
                )
            )
    left = jnp.concatenate(lefts, axis=1)
    chosen = jnp.concatenate(chosen, axis=1)
    right_rows = jnp.concatenate([chosen, chosen, jnp.concatenate(rights, axis=1)], axis=0)
    table = nt_dot(left, right_rows, HIGH)
    width = table.shape[1]
    lane = iota((count, width), 1)
    merged = jnp.where(
        lane < count,
        table[:count],
        jnp.where(lane < 2 * count, table[count : 2 * count], table[2 * count :]),
    )
    out_ref[...] = jnp.concatenate([merged, inner_ref[:, width:]], axis=1)


def pack(total, fold):
    width = LANES // fold
    row, lane = iota(total.shape, 0), iota(total.shape, 1)
    kept = jnp.where(lane < width, total, 0.0)
    moved = kept
    for k in range(1, fold):
        moved = jnp.where(row % fold == k, pltpu.roll(kept, k * width, 1), moved)
    return jnp.concatenate(
        [
            jnp.sum(moved[k : k + fold], axis=0, keepdims=True)
            for k in range(0, total.shape[0], fold)
        ],
        axis=0,
    )


def unpack(packed, fold):
    width = LANES // fold
    rows = packed.shape[0]
    spread = jnp.concatenate(
        [jnp.broadcast_to(packed[k : k + 1], (fold, LANES)) for k in range(rows)], axis=0
    )
    row, lane = iota(spread.shape, 0), iota(spread.shape, 1)
    moved = spread
    for k in range(1, fold):
        moved = jnp.where(row % fold == k, pltpu.roll(spread, LANES - k * width, 1), moved)
    return jnp.where(lane < width, moved, 0.0)


def last_kernel(
    fold, partial_ref, first_in, second_in, c_high, c_low, below_ref, above_ref, sums_ref, *refs
):
    earlier, (payload_ref, wide_ref) = refs[:-2], refs[-2:]
    result = couple(
        partial_ref, first_in, second_in, c_high, c_low, below_ref, above_ref, wide_ref
    )
    vectors = [load(ref) for ref in earlier[: ITERS - 1]]
    total = sums_ref[...]
    count = total.shape[0]
    row, lane = iota(total.shape, 0), iota(total.shape, 1)
    base = 2 * count
    last = ITERS - 1
    pairs = [(index, last, vector, result) for index, vector in enumerate(vectors)]
    pairs += [(last, last, result, result), (last, ITERS, result, load(earlier[last]))]
    for at_row, at_col, left, right in pairs:
        real = left[0] * right[0] + left[1] * right[1]
        imag = left[0] * right[1] - left[1] * right[0]
        for part, value in enumerate((real, imag)):
            value = jnp.sum(jnp.sum(value, axis=0, keepdims=True), axis=1, keepdims=True)
            spot = (row == at_row) & (lane == base + part * count + at_col)
            total = jnp.where(spot, value, total)
    if fold > 1:
        total = pack(total, fold)

    @pl.loop(0, payload_ref.shape[0])
    def _(device):
        payload_ref[device] = total


def settle(
    total_rows, sums, inner, basis_ref, images, previous,
):
    count = sums.shape[0]
    half = count // 2
    shape = sums.shape

    def column(lane, table=sums):
        return jnp.broadcast_to(table[:, lane : lane + 1], shape)

    def cell(row, lane):
        return jnp.broadcast_to(column(lane)[row : row + 1], shape)

    def entry(row, col):
        base = 2 * count
        return cell(row, base + col), cell(row, base + count + col)

    gram = {(a, b): entry(a, b) for a in range(ITERS) for b in range(a, ITERS)}
    target = [entry(a, ITERS) for a in range(ITERS)]
    lower, pivots = {}, []
    for col in range(ITERS):
        pivot = gram[col, col][0]
        for mid in range(col):
            real, imag = lower[col, mid]
            pivot = pivot - (real * real + imag * imag) * pivots[mid]
        pivots.append(pivot)
        for row in range(col + 1, ITERS):
            value = conj(gram[col, row])
            for mid in range(col):
                value = csub(value, scale(cmul(lower[row, mid], conj(lower[col, mid])), pivots[mid]))
            lower[row, col] = (value[0] / pivot, value[1] / pivot)
    forward = []
    for row in range(ITERS):
        value = target[row]
        for mid in range(row):
            value = csub(value, cmul(lower[row, mid], forward[mid]))
        forward.append(value)
    solved = [None] * ITERS
    for row in reversed(range(ITERS)):
        value = (forward[row][0] / pivots[row], forward[row][1] / pivots[row])
        for mid in range(row + 1, ITERS):
            value = csub(value, cmul(conj(lower[mid, row]), solved[mid]))
        solved[row] = value

    offset = ITERS + 1
    square = jnp.zeros(shape, F32)
    for a in range(ITERS):
        square = square + (solved[a][0] ** 2 + solved[a][1] ** 2) * entry(offset + a, offset + a)[0]
        for b in range(a + 1, ITERS):
            pair = cmul(conj(solved[a]), solved[b])
            square = square + 2.0 * cmul(pair, entry(offset + a, offset + b))[0]

    projections = []
    for block in range(2):
        base = block * count
        value = None
        for a in range(ITERS):
            term = cmul(solved[a], (column(base + a), column(base + half + a)))
            value = term if value is None else cadd(value, term)
        projections.append(scale(value, 1.0 / total_rows))
    value = None
    for a in range(ITERS):
        term = cmul(solved[a], entry(count - 1, offset + a))
        value = term if value is None else cadd(value, term)
    extra = scale(value, 1.0 / total_rows)

    row, lane = iota(shape, 0), iota(shape, 1)
    first = 4 * count
    span = 4 * count
    first_row = jnp.zeros(shape, F32)
    second_row = jnp.zeros(shape, F32)
    for block in range(2):
        real, imag = projections[block]
        at_real = (lane == first + block * count + row) | (lane == first + span + block * count + row)
        at_imag = (lane == first + 2 * count + block * count + row) | (
            lane == first + span + 2 * count + block * count + row
        )
        first_row = first_row + jnp.where(at_real, real, jnp.where(at_imag, -imag, 0.0))
        second_row = second_row + jnp.where(at_real, imag, jnp.where(at_imag, real, 0.0))
    first_row = jnp.sum(first_row, axis=0, keepdims=True)
    second_row = jnp.sum(second_row, axis=0, keepdims=True)
    upper = lane < first + span
    real_col = jnp.where(upper, projections[0][0], projections[1][0])
    imag_col = jnp.where(upper, projections[0][1], projections[1][1])
    quad = jnp.sum(inner * (real_col * first_row + imag_col * second_row), axis=1, keepdims=True)
    quad = jnp.broadcast_to(quad, shape)
    for block in range(2):
        base = block * count
        real, imag = projections[block]
        cross = cmul(
            cmul((real, -imag), extra), (column(base + half - 1), column(base + count - 1))
        )[0]
        quad = quad + 2.0 * cross - 2.0 * total_rows * (real * real + imag * imag)
    quad = jnp.broadcast_to(jnp.sum(quad, axis=0, keepdims=True), shape)
    extra_size = extra[0] * extra[0] + extra[1] * extra[1]
    quad = quad + extra_size * (entry(count - 1, count - 1)[0] - 2.0 * total_rows)
    norm = jnp.sqrt((square + quad) * (1.0 / total_rows) + EPSILON)

    coef = tuple(
        jnp.concatenate([projections[0][part], projections[1][part]], axis=0) for part in range(2)
    )
    mixed = cadd(mix_basis(coef, basis_ref), cmul(extra, previous))
    made = None
    for a in range(ITERS):
        term = cmul(solved[a], images[a])
        made = term if made is None else cadd(made, term)
    remain = csub(made, mixed)
    latest = (remain[0] / norm, remain[1] / norm)

    rows = []
    for part in range(2):
        spread = jnp.zeros(shape, F32)
        for block in range(2):
            spread = spread + jnp.where(lane == block * count + row, projections[block][part], 0.0)
        spread = jnp.sum(spread, axis=0, keepdims=True)
        spread = spread + jnp.where(lane[:1] == 2 * count, extra[part][:1], 0.0)
        if part == 0:
            spread = spread + jnp.where(lane[:1] == 2 * count + 1, norm[:1], 0.0)
        rows.append(spread)
    return latest, jnp.concatenate(rows, axis=0)


def reduce_sums(sums_ref):
    if sums_ref.shape[0] <= 64:
        values = [sums_ref[k] for k in range(sums_ref.shape[0])]
        while len(values) > 1:
            values = [
                values[k] + values[k + 1] if k + 1 < len(values) else values[k]
                for k in range(0, len(values), 2)
            ]
        return values[0]
    return jnp.sum(sums_ref[...], axis=0)


def between_kernel(
    total_rows, step, sums_ref, basis_ref, compact_ref, weights_ref, fresh_ref, p_high, p_low,
    *refs,
):
    images = [load(ref) for ref in refs[:ITERS]]
    previous_ref = refs[ITERS]
    (right_ref, image_ref, first_ref, second_ref, latest_ref, coeffs_ref, inner_ref, wide_ref) = refs[
        ITERS + 1 :
    ]
    sums = reduce_sums(sums_ref)
    inner_ref[...] = sums
    latest, coeffs = settle(total_rows, sums, sums, basis_ref, images, load(previous_ref))
    save(latest_ref, latest)
    coeffs_ref[...] = coeffs
    coef, gamma = coefficients(step + 1, compact_ref, weights_ref, fresh_ref)
    right = cadd(mix_basis(coef, basis_ref), cmul(gamma, latest))
    save(right_ref, right)
    image = precondition(right, p_high, p_low, wide_ref)
    save(image_ref, image)
    send(image, first_ref, second_ref)


def finish_kernel(total_rows, sums_ref, inner_ref, basis_ref, *refs):
    images = [load(ref) for ref in refs[:ITERS]]
    previous_ref, before_ref, made_ref, listed_ref = refs[ITERS:]
    sums = unpack(reduce_sums(sums_ref), FOLD)
    previous = load(previous_ref)
    latest, coeffs = settle(total_rows, sums, inner_ref[...], basis_ref, images, previous)
    for step, vector in enumerate((previous, latest)):
        for part in range(2):
            for tile in range(vector[part].shape[0]):
                made_ref[step, part : part + 1, tile * LANES : (tile + 1) * LANES] = vector[part][
                    tile : tile + 1
                ]
    width = listed_ref.shape[2]
    listed_ref[0] = before_ref[:, :width]
    listed_ref[1] = coeffs[:, :width]


def vmem():
    return pl.BlockSpec(memory_space=pltpu.VMEM)


def hbm():
    return pl.BlockSpec(memory_space=pltpu.HBM)


def smem():
    return pl.BlockSpec(memory_space=pltpu.SMEM)


def in_hbm(*arrays):
    return tuple(pltpu.with_memory_space_constraint(array, pltpu.HBM) for array in arrays)


def call(kernel, out_shape, in_specs, scratch, args, flops=10**7):
    return pl.pallas_call(
        kernel,
        out_shape=out_shape,
        in_specs=in_specs,
        out_specs=jax.tree.map(lambda _: vmem(), out_shape),
        scratch_shapes=scratch,
        cost_estimate=pl.CostEstimate(flops=flops, bytes_accessed=10**6, transcendentals=0),
        compiler_params=pltpu.CompilerParams(vmem_limit_bytes=VMEM_LIMIT),
    )(*args)


def local(
    n_dom,
    n_sub,
    basis,
    compact,
    weights,
    fresh,
    shifts,
    k_tiles,
    pattern,
    mass,
    precond,
    c_tiles,
    c_rows,
    c_side,
    c_count,
):
    tiles, slots_k, tile = k_tiles.shape[0], k_tiles.shape[1], k_tiles.shape[2]
    slots = c_tiles.shape[0]
    devices = n_dom * n_sub
    total_rows = float(tiles * tile * devices)
    steps = weights.shape[0]
    vec = jax.ShapeDtypeStruct((2 * tiles, tile), F32)
    edge = jax.ShapeDtypeStruct((2, tile), F32)
    square = jax.ShapeDtypeStruct((tiles, tile), F32)
    k_blocks = tiles * slots_k
    p_blocks = 2 * tiles
    k_part = jax.ShapeDtypeStruct((tile, k_blocks * tile), BF16)
    c_part = jax.ShapeDtypeStruct((tile, slots * tile), BF16)
    p_part = jax.ShapeDtypeStruct((tile, p_blocks * tile), BF16)
    mask = jax.ShapeDtypeStruct((slots, tiles, tile), F32)
    pick = jax.ShapeDtypeStruct(((slots_k - 1) * tiles, tiles * n_sub), BF16)
    drag = jax.ShapeDtypeStruct((steps, 2, tiles, tile), F32)
    compact = jnp.swapaxes(compact, 1, 2)
    pattern = pattern.T
    mass = mass.reshape(tiles, tile)
    zero = jnp.zeros((2 * tiles, tile), F32)

    def wide(blocks):
        return pltpu.VMEM((4 * tiles, blocks * tile), BF16)

    even_swap = [(i, i ^ 1) for i in range(n_dom)]
    odd_swap = []
    for i in range(n_dom):
        other = i + 1 if i % 2 else i - 1
        for j in range(n_sub):
            inside = 0 <= other < n_dom
            target = other * n_sub + j if inside else i * n_sub + (j ^ 1)
            odd_swap.append((i * n_sub + j, target))

    def exchange(image, first, second):
        second = lax.ppermute(second, AXES, odd_swap)
        first = lax.ppermute(first, "dom", even_swap)
        blocks = []
        for k in range(1, n_sub):
            blocks.append(lax.ppermute(image, "sub", [(i, i ^ k) for i in range(n_sub)]))
        return blocks, first, second

    copied = (
        basis, compact, weights, fresh, pattern, c_rows.reshape(1, slots), c_side.reshape(1, slots),
        shifts, mass, k_tiles, c_tiles,
    )
    (right, image, first, second, p_high, p_low, *copied) = call(
        start_kernel,
        (vec, vec, edge, edge, p_part, p_part)
        + tuple(pltpu.VMEM(array.shape, array.dtype) for array in copied),
        [hbm()] * (len(copied) + 1),
        [
            wide(p_blocks),
            pltpu.VMEM(precond.shape, F32),
            pltpu.SemaphoreType.DMA((len(copied),)),
            pltpu.SemaphoreType.DMA((tiles,)),
        ],
        in_hbm(*copied, precond),
    )
    basis, compact, weights, fresh = copied[:4]
    k_high, k_low, c_high, c_low, pick_table, below, above, drag = call(
        functools.partial(prepare_kernel, n_dom),
        (k_part, k_part, c_part, c_part, pick, mask, mask, drag),
        [smem()] + [vmem()] * 7, [], (c_count, *copied[4:]),
    )
    previous = zero
    for step in range(steps):
        term = right
        images, results = [image], []
        for index in range(ITERS):
            blocks, first_in, second_in = exchange(image, first, second)
            ahead = ()
            if step == 0 and index == ITERS - 2:
                inner = call(inner_kernel, square, [vmem()] * 2, [], (basis, image))
                ahead = (inner,)
            partial = call(
                functools.partial(stiff_kernel, step, n_sub - 1), vec,
                [vmem()] * (n_sub + 4 + len(ahead)), [wide(k_blocks)],
                (image, *blocks, drag, k_high, k_low, pick_table, *ahead),
            )
            common = (partial, first_in, second_in, c_high, c_low, below, above)
            if index + 1 < ITERS:
                later = [vec] if index + 2 < ITERS else []
                result, image, first, second, *later = call(
                    level_kernel, (vec, vec, edge, edge, *later), [vmem()] * 10,
                    [wide(max(slots, p_blocks))], common + (term, p_high, p_low),
                )
                term = later[0] if later else None
                results.append(result)
                images.append(image)
            else:
                sums = call(
                    gram_kernel, square, [vmem()] * (3 + 2 * ITERS),
                    [pltpu.VMEM((tiles, 4 * tiles, tile), F32)],
                    (basis, previous, inner, *results, right, *images),
                )
                fold = FOLD if step + 1 == steps else 1
                payload = call(
                    functools.partial(last_kernel, fold),
                    jax.ShapeDtypeStruct((devices, tiles // fold, tile), F32),
                    [vmem()] * (8 + ITERS), [wide(slots)], common + (sums, *results, right),
                )
        sums = lax.all_to_all(payload, AXES, 0, 0)
        if step + 1 < steps:
            right, image, first, second, latest, coeffs, inner_sum = call(
                functools.partial(between_kernel, total_rows, step),
                (vec, vec, edge, edge, vec, jax.ShapeDtypeStruct((2, tile), F32), square),
                [vmem()] * (8 + ITERS), [wide(p_blocks)],
                (sums, basis, compact, weights, fresh, p_high, p_low, *images, previous),
            )
            previous = latest
        else:
            width = basis.shape[1] + 2
            made, listed = call(
                functools.partial(finish_kernel, total_rows),
                (
                    jax.ShapeDtypeStruct((steps, 2, tiles * tile), F32),
                    jax.ShapeDtypeStruct((steps, 2, width), F32),
                ),
                [vmem()] * (5 + ITERS), [],
                (sums, inner_sum, basis, *images, previous, coeffs),
            )
    return made, listed


def solution(mesh):
    placed = (
        P(None, None, AXES),
        P(),
        P(),
        P(),
        P(),
        P(AXES, None, None, None),
        P(AXES, None),
        P(AXES),
        P(AXES, None, None, None),
        P(AXES, None, None),
        P(AXES),
        P(AXES),
        P(AXES),
    )
    return jax.shard_map(
        functools.partial(local, mesh.shape["dom"], mesh.shape["sub"]),
        mesh=mesh,
        in_specs=placed,
        out_specs=(P(None, None, AXES), P()),
        check_vma=False,
    )
```

```python
import functools
import jax
import jax.numpy as jnp
from jax import lax
from jax.experimental import pallas as pl
from jax.experimental.pallas import tpu as pltpu
from jax.sharding import PartitionSpec as P

ITERS = 3
EPSILON = 1e-06
HIGH = lax.Precision.HIGHEST
F32 = jnp.float32
BF16 = jnp.bfloat16
NT_DIMS = (((1,), (1,)), ((), ()))
LANES = 128
COPIED = 11
FOLDS = (2, 4)
VMEM_LIMIT = 12 * 1024 * 1024
AXES = ("dom", "sub")


def iota(shape, dim):
    return lax.broadcasted_iota(jnp.int32, shape, dim)


def split(x):
    high = x.astype(BF16).astype(F32)
    return high, x - high


def cmul(a, b):
    return a[0] * b[0] - a[1] * b[1], a[0] * b[1] + a[1] * b[0]


def conj(a):
    return a[0], -a[1]


def csub(a, b):
    return a[0] - b[0], a[1] - b[1]


def cadd(a, b):
    return a[0] + b[0], a[1] + b[1]


def scale(a, s):
    return a[0] * s, a[1] * s


def nt_dot(a, b, precision=None):
    return lax.dot_general(a, b, NT_DIMS, precision=precision, preferred_element_type=F32)


def store_parts(high_ref, low_ref, block, x):
    lanes = slice(block * LANES, (block + 1) * LANES)
    high, low = split(x)
    high_ref[:, lanes] = high.astype(BF16)
    low_ref[:, lanes] = low.astype(BF16)


def product(high_ref, low_ref, wide_ref, blocks):
    lanes = blocks * LANES
    wide = wide_ref[:, :lanes]
    total = nt_dot(high_ref[...], wide) + nt_dot(low_ref[...], wide)
    flipped = total.T
    rows = flipped.shape[0] // 4
    parts = [flipped[k * rows : (k + 1) * rows] for k in range(4)]
    return parts[0] + parts[2], parts[1] + parts[3]


def put(wide_ref, block, parts):
    wide_ref[:, block * LANES : (block + 1) * LANES] = jnp.concatenate(parts, axis=0).astype(BF16)


def parts_of(vector):
    real, imag = vector
    real_high, real_low = split(real)
    imag_high, imag_low = split(imag)
    return [real_high, imag_high, real_low, imag_low]


def precondition(vector, high_ref, low_ref, wide_ref):
    tiles = vector[0].shape[0]
    straight = parts_of(vector)
    turned = [-straight[1], straight[0], -straight[3], straight[2]]
    row = iota(vector[0].shape, 0)
    for tile in range(tiles):
        mask = row == tile
        put(wide_ref, 2 * tile, [jnp.where(mask, x, 0.0) for x in straight])
        put(wide_ref, 2 * tile + 1, [jnp.where(mask, x, 0.0) for x in turned])
    return product(high_ref, low_ref, wide_ref, 2 * tiles)


def load(ref):
    rows = ref.shape[0] // 2
    return ref[:rows], ref[rows:]


def save(ref, vector):
    ref[...] = jnp.concatenate(vector, axis=0)


def send(vector, first_ref, second_ref):
    even = lax.rem(lax.axis_index("dom"), 2) == 0
    rows = vector[0].shape[0]
    head = jnp.concatenate([vector[0][:1], vector[1][:1]], axis=0)
    tail = jnp.concatenate([vector[0][rows - 1 :], vector[1][rows - 1 :]], axis=0)
    first_ref[...] = jnp.where(even, tail, head)
    second_ref[...] = jnp.where(even, head, tail)


def mix_basis(coef, basis_ref):
    real, imag = coef
    tiles = basis_ref.shape[2] // LANES
    row = iota((tiles, LANES), 0)
    out_real = jnp.zeros((tiles, LANES), F32)
    out_imag = jnp.zeros((tiles, LANES), F32)
    for tile in range(tiles):
        lanes = slice(tile * LANES, (tile + 1) * LANES)
        base_real, base_imag = basis_ref[0, :, lanes], basis_ref[1, :, lanes]
        sum_real = jnp.sum(real * base_real - imag * base_imag, axis=0, keepdims=True)
        sum_imag = jnp.sum(real * base_imag + imag * base_real, axis=0, keepdims=True)
        out_real = jnp.where(row == tile, sum_real, out_real)
        out_imag = jnp.where(row == tile, sum_imag, out_imag)
    return out_real, out_imag


def coefficients(step, compact_ref, weights_ref, fresh_ref):
    beta = weights_ref[step]
    beta_real, beta_imag = beta[0:1], beta[1:2]
    compact_real, compact_imag = compact_ref[0], compact_ref[1]
    coef_real = jnp.sum(compact_real * beta_real - compact_imag * beta_imag, axis=1, keepdims=True)
    coef_imag = jnp.sum(compact_imag * beta_real + compact_real * beta_imag, axis=1, keepdims=True)
    fresh = fresh_ref[...]
    gamma_real = jnp.sum(beta_real * fresh[0:1] - beta_imag * fresh[1:2], axis=1, keepdims=True)
    gamma_imag = jnp.sum(beta_real * fresh[1:2] + beta_imag * fresh[0:1], axis=1, keepdims=True)
    return (coef_real, coef_imag), (gamma_real, gamma_imag)


def start_kernel(*refs):
    sources, refs = refs[:COPIED], refs[COPIED:]
    precond_in, refs = refs[0], refs[1:]
    right_ref, image_ref, first_ref, second_ref, high_ref, low_ref = refs[:6]
    targets, refs = refs[6 : 6 + COPIED], refs[6 + COPIED :]
    wide_ref, precond_ref, small_sem, tile_sem = refs
    moves = [
        pltpu.make_async_copy(source, target, small_sem.at[index])
        for index, (source, target) in enumerate(zip(sources, targets))
    ]
    tiles = precond_in.shape[0]
    tile_moves = [
        pltpu.make_async_copy(precond_in.at[tile], precond_ref.at[tile], tile_sem.at[tile])
        for tile in range(tiles)
    ]
    early, late = moves[:4], moves[4:]
    for move in early + tile_moves + late:
        move.start()
    for move in early:
        move.wait()
    basis_ref, compact_ref, weights_ref, fresh_ref = targets[:4]
    coef, _ = coefficients(0, compact_ref, weights_ref, fresh_ref)
    right = mix_basis(coef, basis_ref)
    save(right_ref, right)
    for tile in range(tiles):
        tile_moves[tile].wait()
        for part in range(2):
            store_parts(high_ref, low_ref, 2 * tile + part, precond_ref[tile, part])
    image = precondition(right, high_ref, low_ref, wide_ref)
    save(image_ref, image)
    send(image, first_ref, second_ref)
    for move in late:
        move.wait()


def as_column(row):
    count = row.shape[1]
    same = iota((count, count), 0) == iota((count, count), 1)
    return jnp.sum(jnp.where(same, row, 0.0), axis=1, keepdims=True)


def prepare_kernel(
    n_dom, count_ref, pattern_ref, rows_ref, side_ref, shifts_ref, mass_ref, k_ref, c_ref,
    high_ref, low_ref, c_high_ref, c_low_ref, pick_ref, below_ref, above_ref, drag_ref,
):
    tiles, slots_k, slots = k_ref.shape[0], k_ref.shape[1], c_ref.shape[0]
    for tile in range(tiles):
        for slot in range(slots_k):
            store_parts(high_ref, low_ref, tile * slots_k + slot, k_ref[tile, slot])
    for slot in range(slots):
        store_parts(c_high_ref, c_low_ref, slot, c_ref[slot])
    mine = lax.axis_index("sub") * tiles
    lane = iota((tiles, pick_ref.shape[1]), 1) ^ mine
    lane = lane.astype(F32)
    picked = [
        jnp.where(as_column(pattern_ref[slot : slot + 1].astype(F32)) == lane, 1.0, 0.0)
        for slot in range(slots_k - 1)
    ]
    pick_ref[...] = jnp.concatenate(picked, axis=0).astype(BF16)
    domain = lax.axis_index("dom")
    shape = (tiles, LANES)
    row = iota(shape, 0)
    for slot in range(slots):
        live = slot < count_ref[0]
        side = jnp.broadcast_to(side_ref[:, slot : slot + 1], shape)
        here = row == jnp.broadcast_to(rows_ref[:, slot : slot + 1], shape)
        low_on = jnp.where(live & (domain > 0), 1.0, 0.0)
        high_on = jnp.where(live & (domain < n_dom - 1), 1.0, 0.0)
        below_ref[slot] = jnp.where(here & (side == 0), low_on, 0.0)
        above_ref[slot] = jnp.where(here & (side != 0), high_on, 0.0)
    mass = mass_ref[...]
    for step in range(drag_ref.shape[0]):
        for part in range(2):
            shift = jnp.broadcast_to(shifts_ref[step : step + 1, part : part + 1], shape)
            drag_ref[step, part] = mass * shift


def inner_kernel(basis_ref, after_ref, inner_ref):
    real, imag = basis_ref[0], basis_ref[1]
    inner = nt_dot(real, jnp.concatenate([real, imag], axis=0), HIGH)
    inner = inner + nt_dot(imag, jnp.concatenate([imag, -real], axis=0), HIGH)
    half = inner_ref.shape[0]
    row, lane = iota((half, half), 0), iota((half, half), 1)

    def block(left, right, part):
        lanes = (2 * part + right) * half
        return inner[left * half : (left + 1) * half, lanes : lanes + half]

    low_real = block(1, 1, 0)
    pieces = [
        jnp.where(lane >= row, block(0, 0, 0), low_real),
        jnp.where(lane > row, block(0, 0, 1), jnp.where(lane < row, block(1, 1, 1), low_real)),
        block(0, 1, 0),
        block(0, 1, 1),
    ]
    inner_ref[...] = jnp.zeros(inner_ref.shape, F32)
    for index, piece in enumerate(pieces):
        inner_ref[:, (4 + index) * half : (5 + index) * half] = piece


def stiff_kernel(step, others, image_ref, *refs):
    blocks, (drag_ref, high_ref, low_ref, pick_ref) = refs[:others], refs[others : others + 4]
    result_ref, wide_ref = refs[-2:]
    image = load(image_ref)
    tiles = image[0].shape[0]
    own = parts_of(image)
    gathered = [own] + [parts_of(load(block)) for block in blocks]
    table = jnp.concatenate(
        [jnp.concatenate([g[part] for g in gathered], axis=0) for part in range(4)], axis=1
    ).astype(BF16)
    chosen = jnp.dot(pick_ref[...], table, preferred_element_type=F32)
    others = chosen.shape[0] // tiles
    row = iota(image[0].shape, 0)
    for tile in range(tiles):
        mask = row == tile
        base = tile * (others + 1)
        put(wide_ref, base, [jnp.where(mask, x, 0.0) for x in own])
        for slot in range(others):
            rows = slice(slot * tiles, (slot + 1) * tiles)
            put(
                wide_ref,
                base + 1 + slot,
                [
                    jnp.where(mask, chosen[rows, part * LANES : (part + 1) * LANES], 0.0)
                    for part in range(4)
                ],
            )
    stiff = product(high_ref, low_ref, wide_ref, tiles * (others + 1))
    drag = cmul((drag_ref[step, 0], drag_ref[step, 1]), image)
    save(result_ref, csub(stiff, drag))


def couple(partial_ref, first_ref, second_ref, high_ref, low_ref, below_ref, above_ref, wide_ref):
    even = lax.rem(lax.axis_index("dom"), 2) == 0
    first, second = first_ref[...], second_ref[...]
    below = jnp.where(even, second, first)
    above = jnp.where(even, first, second)
    below = parts_of((below[0:1], below[1:2]))
    above = parts_of((above[0:1], above[1:2]))
    slots = below_ref.shape[0]
    for slot in range(slots):
        low_mask, high_mask = below_ref[slot], above_ref[slot]
        put(wide_ref, slot, [low_mask * below[part] + high_mask * above[part] for part in range(4)])
    return cadd(load(partial_ref), product(high_ref, low_ref, wide_ref, slots))


def level_kernel(
    partial_ref, first_in, second_in, c_high, c_low, below_ref, above_ref, term_ref, p_high, p_low,
    result_ref, out_ref, first_ref, second_ref, *refs,
):
    next_refs, wide_ref = refs[:-1], refs[-1]
    result = couple(
        partial_ref, first_in, second_in, c_high, c_low, below_ref, above_ref, wide_ref
    )
    save(result_ref, result)
    term = csub(result, load(term_ref))
    for next_ref in next_refs:
        save(next_ref, term)
    image = precondition(term, p_high, p_low, wide_ref)
    save(out_ref, image)
    send(image, first_ref, second_ref)


def gram_kernel(basis_ref, previous_ref, inner_ref, *refs):
    refs, (out_ref, rows_ref) = refs[:-2], refs[-2:]
    results = [load(ref) for ref in refs[: ITERS - 1]]
    right = load(refs[ITERS - 1])
    images = [load(ref) for ref in refs[ITERS:]]
    zero = jnp.zeros(right[0].shape, F32)
    vectors = results + [(zero, zero), right] + images + [load(previous_ref)]
    count = len(vectors)
    for index, (real, imag) in enumerate(vectors):
        rows_ref[:, index, :] = real
        rows_ref[:, count + index, :] = imag
        rows_ref[:, 2 * count + index, :] = imag
        rows_ref[:, 3 * count + index, :] = -real
    tiles = rows_ref.shape[0]
    lefts, rights, chosen = [], [], []
    half = count // 2
    for tile in range(tiles):
        lanes = slice(tile * LANES, (tile + 1) * LANES)
        for part in range(2):
            left = rows_ref[tile, part * count : (part + 1) * count]
            lefts.append(jnp.concatenate([basis_ref[part, :, lanes], left], axis=0))
            base = 2 * part * count
            rights.append(rows_ref[tile, base : base + 2 * count])
            chosen.append(
                jnp.concatenate(
                    [
                        rows_ref[tile, base + half : base + count],
                        rows_ref[tile, base + count + half : base + 2 * count],
                    ],
                    axis=0,
                )
            )
    left = jnp.concatenate(lefts, axis=1)
    chosen = jnp.concatenate(chosen, axis=1)
    right_rows = jnp.concatenate([chosen, chosen, jnp.concatenate(rights, axis=1)], axis=0)
    table = nt_dot(left, right_rows, HIGH)
    width = table.shape[1]
    lane = iota((count, width), 1)
    merged = jnp.where(
        lane < count,
        table[:count],
        jnp.where(lane < 2 * count, table[count : 2 * count], table[2 * count :]),
    )
    out_ref[...] = jnp.concatenate([merged, inner_ref[:, width:]], axis=1)


def pack(total, fold):
    width = LANES // fold
    row, lane = iota(total.shape, 0), iota(total.shape, 1)
    kept = jnp.where(lane < width, total, 0.0)
    moved = kept
    for k in range(1, fold):
        moved = jnp.where(row % fold == k, pltpu.roll(kept, k * width, 1), moved)
    return jnp.concatenate(
        [
            jnp.sum(moved[k : k + fold], axis=0, keepdims=True)
            for k in range(0, total.shape[0], fold)
        ],
        axis=0,
    )


def unpack(packed, fold):
    width = LANES // fold
    rows = packed.shape[0]
    spread = jnp.concatenate(
        [jnp.broadcast_to(packed[k : k + 1], (fold, LANES)) for k in range(rows)], axis=0
    )
    row, lane = iota(spread.shape, 0), iota(spread.shape, 1)
    moved = spread
    for k in range(1, fold):
        moved = jnp.where(row % fold == k, pltpu.roll(spread, LANES - k * width, 1), moved)
    return jnp.where(lane < width, moved, 0.0)


def last_kernel(
    fold, partial_ref, first_in, second_in, c_high, c_low, below_ref, above_ref, sums_ref, *refs
):
    earlier, (payload_ref, wide_ref) = refs[:-2], refs[-2:]
    result = couple(
        partial_ref, first_in, second_in, c_high, c_low, below_ref, above_ref, wide_ref
    )
    vectors = [load(ref) for ref in earlier[: ITERS - 1]]
    total = sums_ref[...]
    count = total.shape[0]
    row, lane = iota(total.shape, 0), iota(total.shape, 1)
    base = 2 * count
    last = ITERS - 1
    pairs = [(index, last, vector, result) for index, vector in enumerate(vectors)]
    pairs += [(last, last, result, result), (last, ITERS, result, load(earlier[last]))]
    for at_row, at_col, left, right in pairs:
        real = left[0] * right[0] + left[1] * right[1]
        imag = left[0] * right[1] - left[1] * right[0]
        for part, value in enumerate((real, imag)):
            value = jnp.sum(jnp.sum(value, axis=0, keepdims=True), axis=1, keepdims=True)
            spot = (row == at_row) & (lane == base + part * count + at_col)
            total = jnp.where(spot, value, total)
    total = pack(total, fold)

    @pl.loop(0, payload_ref.shape[0])
    def _(device):
        payload_ref[device] = total


def settle(
    total_rows, sums, inner, basis_ref, images, previous,
):
    count = sums.shape[0]
    half = count // 2
    shape = sums.shape

    def column(lane, table=sums):
        return jnp.broadcast_to(table[:, lane : lane + 1], shape)

    def cell(row, lane):
        return jnp.broadcast_to(column(lane)[row : row + 1], shape)

    def entry(row, col):
        base = 2 * count
        return cell(row, base + col), cell(row, base + count + col)

    gram = {(a, b): entry(a, b) for a in range(ITERS) for b in range(a, ITERS)}
    target = [entry(a, ITERS) for a in range(ITERS)]
    lower, pivots = {}, []
    for col in range(ITERS):
        pivot = gram[col, col][0]
        for mid in range(col):
            real, imag = lower[col, mid]
            pivot = pivot - (real * real + imag * imag) * pivots[mid]
        pivots.append(pivot)
        for row in range(col + 1, ITERS):
            value = conj(gram[col, row])
            for mid in range(col):
                value = csub(value, scale(cmul(lower[row, mid], conj(lower[col, mid])), pivots[mid]))
            lower[row, col] = (value[0] / pivot, value[1] / pivot)
    forward = []
    for row in range(ITERS):
        value = target[row]
        for mid in range(row):
            value = csub(value, cmul(lower[row, mid], forward[mid]))
        forward.append(value)
    solved = [None] * ITERS
    for row in reversed(range(ITERS)):
        value = (forward[row][0] / pivots[row], forward[row][1] / pivots[row])
        for mid in range(row + 1, ITERS):
            value = csub(value, cmul(conj(lower[mid, row]), solved[mid]))
        solved[row] = value

    offset = ITERS + 1
    square = jnp.zeros(shape, F32)
    for a in range(ITERS):
        square = square + (solved[a][0] ** 2 + solved[a][1] ** 2) * entry(offset + a, offset + a)[0]
        for b in range(a + 1, ITERS):
            pair = cmul(conj(solved[a]), solved[b])
            square = square + 2.0 * cmul(pair, entry(offset + a, offset + b))[0]

    projections = []
    for block in range(2):
        base = block * count
        value = None
        for a in range(ITERS):
            term = cmul(solved[a], (column(base + a), column(base + half + a)))
            value = term if value is None else cadd(value, term)
        projections.append(scale(value, 1.0 / total_rows))
    value = None
    for a in range(ITERS):
        term = cmul(solved[a], entry(count - 1, offset + a))
        value = term if value is None else cadd(value, term)
    extra = scale(value, 1.0 / total_rows)

    row, lane = iota(shape, 0), iota(shape, 1)
    spot = lane - 4 * count
    column_of = spot % count
    zone = jnp.where((spot >= 0) & (spot < 4 * count), spot // count, 4)
    spread = [
        [
            jnp.sum(jnp.where(column_of == row, part, 0.0), axis=0, keepdims=True)
            for part in projections[block]
        ]
        for block in range(2)
    ]

    def real_weight(left, right):
        return left[0] * right[0] + left[1] * right[1]

    def imag_weight(left, right):
        return left[1] * right[0] - left[0] * right[1]

    first, second = projections
    same = real_weight(second, spread[1])
    upper, lower = column_of > row, column_of < row
    zones = [
        jnp.where(
            lower,
            2.0 * same,
            jnp.where(upper, 2.0, 1.0) * real_weight(first, spread[0]),
        ),
        jnp.where(
            upper,
            2.0 * imag_weight(first, spread[0]),
            jnp.where(lower, 2.0 * imag_weight(second, spread[1]), same),
        ),
        2.0 * real_weight(first, spread[1]),
        2.0 * imag_weight(first, spread[1]),
    ]
    weight = jnp.zeros(shape, F32)
    for index, value in enumerate(zones):
        weight = jnp.where(zone == index, value, weight)
    quad = jnp.sum(inner * weight, axis=1, keepdims=True)
    quad = jnp.broadcast_to(quad, shape)
    for block in range(2):
        base = block * count
        real, imag = projections[block]
        cross = cmul(
            cmul((real, -imag), extra), (column(base + half - 1), column(base + count - 1))
        )[0]
        quad = quad + 2.0 * cross - 2.0 * total_rows * (real * real + imag * imag)
    quad = jnp.broadcast_to(jnp.sum(quad, axis=0, keepdims=True), shape)
    extra_size = extra[0] * extra[0] + extra[1] * extra[1]
    quad = quad + extra_size * (entry(count - 1, count - 1)[0] - 2.0 * total_rows)
    norm = jnp.sqrt((square + quad) * (1.0 / total_rows) + EPSILON)

    coef = tuple(
        jnp.concatenate([projections[0][part], projections[1][part]], axis=0) for part in range(2)
    )
    mixed = cadd(mix_basis(coef, basis_ref), cmul(extra, previous))
    made = None
    for a in range(ITERS):
        term = cmul(solved[a], images[a])
        made = term if made is None else cadd(made, term)
    remain = csub(made, mixed)
    latest = (remain[0] / norm, remain[1] / norm)

    rows = []
    for part in range(2):
        spread = jnp.zeros(shape, F32)
        for block in range(2):
            spread = spread + jnp.where(lane == block * count + row, projections[block][part], 0.0)
        spread = jnp.sum(spread, axis=0, keepdims=True)
        spread = spread + jnp.where(lane[:1] == 2 * count, extra[part][:1], 0.0)
        if part == 0:
            spread = spread + jnp.where(lane[:1] == 2 * count + 1, norm[:1], 0.0)
        rows.append(spread)
    return latest, jnp.concatenate(rows, axis=0)


def reduce_sums(sums_ref):
    if sums_ref.shape[0] <= 64:
        values = [sums_ref[k] for k in range(sums_ref.shape[0])]
        while len(values) > 1:
            values = [
                values[k] + values[k + 1] if k + 1 < len(values) else values[k]
                for k in range(0, len(values), 2)
            ]
        return values[0]
    return jnp.sum(sums_ref[...], axis=0)


def between_kernel(
    total_rows, step, sums_ref, basis_ref, compact_ref, weights_ref, fresh_ref, p_high, p_low,
    *refs,
):
    images = [load(ref) for ref in refs[:ITERS]]
    previous_ref = refs[ITERS]
    (right_ref, image_ref, first_ref, second_ref, latest_ref, coeffs_ref, inner_ref, wide_ref) = refs[
        ITERS + 1 :
    ]
    sums = unpack(reduce_sums(sums_ref), FOLDS[step])
    inner_ref[...] = sums
    latest, coeffs = settle(total_rows, sums, sums, basis_ref, images, load(previous_ref))
    save(latest_ref, latest)
    coeffs_ref[...] = coeffs
    coef, gamma = coefficients(step + 1, compact_ref, weights_ref, fresh_ref)
    right = cadd(mix_basis(coef, basis_ref), cmul(gamma, latest))
    save(right_ref, right)
    image = precondition(right, p_high, p_low, wide_ref)
    save(image_ref, image)
    send(image, first_ref, second_ref)


def finish_kernel(total_rows, sums_ref, inner_ref, basis_ref, *refs):
    images = [load(ref) for ref in refs[:ITERS]]
    previous_ref, before_ref, made_ref, listed_ref = refs[ITERS:]
    sums = unpack(reduce_sums(sums_ref), FOLDS[-1])
    previous = load(previous_ref)
    latest, coeffs = settle(total_rows, sums, inner_ref[...], basis_ref, images, previous)
    for step, vector in enumerate((previous, latest)):
        for part in range(2):
            for tile in range(vector[part].shape[0]):
                made_ref[step, part : part + 1, tile * LANES : (tile + 1) * LANES] = vector[part][
                    tile : tile + 1
                ]
    width = listed_ref.shape[2]
    listed_ref[0] = before_ref[:, :width]
    listed_ref[1] = coeffs[:, :width]


def vmem():
    return pl.BlockSpec(memory_space=pltpu.VMEM)


def hbm():
    return pl.BlockSpec(memory_space=pltpu.HBM)


def smem():
    return pl.BlockSpec(memory_space=pltpu.SMEM)


def in_hbm(*arrays):
    return tuple(pltpu.with_memory_space_constraint(array, pltpu.HBM) for array in arrays)


def call(kernel, out_shape, in_specs, scratch, args, flops=10**7):
    return pl.pallas_call(
        kernel,
        out_shape=out_shape,
        in_specs=in_specs,
        out_specs=jax.tree.map(lambda _: vmem(), out_shape),
        scratch_shapes=scratch,
        cost_estimate=pl.CostEstimate(flops=flops, bytes_accessed=10**6, transcendentals=0),
        compiler_params=pltpu.CompilerParams(vmem_limit_bytes=VMEM_LIMIT),
    )(*args)


def local(
    n_dom,
    n_sub,
    basis,
    compact,
    weights,
    fresh,
    shifts,
    k_tiles,
    pattern,
    mass,
    precond,
    c_tiles,
    c_rows,
    c_side,
    c_count,
):
    tiles, slots_k, tile = k_tiles.shape[0], k_tiles.shape[1], k_tiles.shape[2]
    slots = c_tiles.shape[0]
    devices = n_dom * n_sub
    total_rows = float(tiles * tile * devices)
    steps = weights.shape[0]
    vec = jax.ShapeDtypeStruct((2 * tiles, tile), F32)
    edge = jax.ShapeDtypeStruct((2, tile), F32)
    square = jax.ShapeDtypeStruct((tiles, tile), F32)
    k_blocks = tiles * slots_k
    p_blocks = 2 * tiles
    k_part = jax.ShapeDtypeStruct((tile, k_blocks * tile), BF16)
    c_part = jax.ShapeDtypeStruct((tile, slots * tile), BF16)
    p_part = jax.ShapeDtypeStruct((tile, p_blocks * tile), BF16)
    mask = jax.ShapeDtypeStruct((slots, tiles, tile), F32)
    pick = jax.ShapeDtypeStruct(((slots_k - 1) * tiles, tiles * n_sub), BF16)
    drag = jax.ShapeDtypeStruct((steps, 2, tiles, tile), F32)
    compact = jnp.swapaxes(compact, 1, 2)
    pattern = pattern.T
    mass = mass.reshape(tiles, tile)
    zero = jnp.zeros((2 * tiles, tile), F32)

    def wide(blocks):
        return pltpu.VMEM((4 * tiles, blocks * tile), BF16)

    even_swap = [(i, i ^ 1) for i in range(n_dom)]
    odd_swap = []
    for i in range(n_dom):
        other = i + 1 if i % 2 else i - 1
        for j in range(n_sub):
            inside = 0 <= other < n_dom
            target = other * n_sub + j if inside else i * n_sub + (j ^ 1)
            odd_swap.append((i * n_sub + j, target))

    def exchange(image, first, second):
        second = lax.ppermute(second, AXES, odd_swap)
        first = lax.ppermute(first, "dom", even_swap)
        blocks = []
        for k in range(1, n_sub):
            blocks.append(lax.ppermute(image, "sub", [(i, i ^ k) for i in range(n_sub)]))
        return blocks, first, second

    copied = (
        basis, compact, weights, fresh, pattern, c_rows.reshape(1, slots), c_side.reshape(1, slots),
        shifts, mass, k_tiles, c_tiles,
    )
    (right, image, first, second, p_high, p_low, *copied) = call(
        start_kernel,
        (vec, vec, edge, edge, p_part, p_part)
        + tuple(pltpu.VMEM(array.shape, array.dtype) for array in copied),
        [hbm()] * (len(copied) + 1),
        [
            wide(p_blocks),
            pltpu.VMEM(precond.shape, F32),
            pltpu.SemaphoreType.DMA((len(copied),)),
            pltpu.SemaphoreType.DMA((tiles,)),
        ],
        in_hbm(*copied, precond),
    )
    basis, compact, weights, fresh = copied[:4]
    k_high, k_low, c_high, c_low, pick_table, below, above, drag = call(
        functools.partial(prepare_kernel, n_dom),
        (k_part, k_part, c_part, c_part, pick, mask, mask, drag),
        [smem()] + [vmem()] * 7, [], (c_count, *copied[4:]),
    )
    previous = zero
    for step in range(steps):
        term = right
        images, results = [image], []
        for index in range(ITERS):
            blocks, first_in, second_in = exchange(image, first, second)
            ahead = ()
            if step == 0 and index == ITERS - 2:
                inner = call(inner_kernel, square, [vmem()] * 2, [], (basis, image))
                ahead = (inner,)
            partial = call(
                functools.partial(stiff_kernel, step, n_sub - 1), vec,
                [vmem()] * (n_sub + 4 + len(ahead)), [wide(k_blocks)],
                (image, *blocks, drag, k_high, k_low, pick_table, *ahead),
            )
            common = (partial, first_in, second_in, c_high, c_low, below, above)
            if index + 1 < ITERS:
                later = [vec] if index + 2 < ITERS else []
                result, image, first, second, *later = call(
                    level_kernel, (vec, vec, edge, edge, *later), [vmem()] * 10,
                    [wide(max(slots, p_blocks))], common + (term, p_high, p_low),
                )
                term = later[0] if later else None
                results.append(result)
                images.append(image)
            else:
                sums = call(
                    gram_kernel, square, [vmem()] * (3 + 2 * ITERS),
                    [pltpu.VMEM((tiles, 4 * tiles, tile), F32)],
                    (basis, previous, inner, *results, right, *images),
                )
                fold = FOLDS[step]
                payload = call(
                    functools.partial(last_kernel, fold),
                    jax.ShapeDtypeStruct((devices, tiles // fold, tile), F32),
                    [vmem()] * (8 + ITERS), [wide(slots)], common + (sums, *results, right),
                )
        sums = lax.all_to_all(payload, AXES, 0, 0)
        if step + 1 < steps:
            right, image, first, second, latest, coeffs, inner_sum = call(
                functools.partial(between_kernel, total_rows, step),
                (vec, vec, edge, edge, vec, jax.ShapeDtypeStruct((2, tile), F32), square),
                [vmem()] * (8 + ITERS), [wide(p_blocks)],
                (sums, basis, compact, weights, fresh, p_high, p_low, *images, previous),
            )
            previous = latest
        else:
            width = basis.shape[1] + 2
            made, listed = call(
                functools.partial(finish_kernel, total_rows),
                (
                    jax.ShapeDtypeStruct((steps, 2, tiles * tile), F32),
                    jax.ShapeDtypeStruct((steps, 2, width), F32),
                ),
                [vmem()] * (5 + ITERS), [],
                (sums, inner_sum, basis, *images, previous, coeffs),
            )
    return made, listed


def solution(mesh):
    placed = (
        P(None, None, AXES),
        P(),
        P(),
        P(),
        P(),
        P(AXES, None, None, None),
        P(AXES, None),
        P(AXES),
        P(AXES, None, None, None),
        P(AXES, None, None),
        P(AXES),
        P(AXES),
        P(AXES),
    )
    return jax.shard_map(
        functools.partial(local, mesh.shape["dom"], mesh.shape["sub"]),
        mesh=mesh,
        in_specs=placed,
        out_specs=(P(None, None, AXES), P()),
        check_vma=False,
    )
```

```python
import functools
import jax
import jax.numpy as jnp
from jax import lax
from jax.experimental import pallas as pl
from jax.experimental.pallas import tpu as pltpu
from jax.sharding import PartitionSpec as P

ITERS = 3
EPSILON = 1e-06
HIGH = lax.Precision.HIGHEST
F32 = jnp.float32
BF16 = jnp.bfloat16
NT_DIMS = (((1,), (1,)), ((), ()))
LANES = 128
COPIED = 10
FOLDS = (2, 4)
VMEM_LIMIT = 12 * 1024 * 1024
AXES = ("dom", "sub")


def iota(shape, dim):
    return lax.broadcasted_iota(jnp.int32, shape, dim)


def split(x):
    high = x.astype(BF16).astype(F32)
    return high, x - high


def cmul(a, b):
    return a[0] * b[0] - a[1] * b[1], a[0] * b[1] + a[1] * b[0]


def conj(a):
    return a[0], -a[1]


def csub(a, b):
    return a[0] - b[0], a[1] - b[1]


def cadd(a, b):
    return a[0] + b[0], a[1] + b[1]


def scale(a, s):
    return a[0] * s, a[1] * s


def nt_dot(a, b, precision=None):
    return lax.dot_general(a, b, NT_DIMS, precision=precision, preferred_element_type=F32)


def store_parts(high_ref, low_ref, block, x):
    lanes = slice(block * LANES, (block + 1) * LANES)
    high, low = split(x)
    high_ref[:, lanes] = high.astype(BF16)
    low_ref[:, lanes] = low.astype(BF16)


def product(high_ref, low_ref, wide_ref, blocks):
    lanes = blocks * LANES
    wide = wide_ref[:, :lanes]
    total = nt_dot(high_ref[...], wide) + nt_dot(low_ref[...], wide)
    flipped = total.T
    rows = flipped.shape[0] // 4
    parts = [flipped[k * rows : (k + 1) * rows] for k in range(4)]
    return parts[0] + parts[2], parts[1] + parts[3]


def put(wide_ref, block, parts):
    wide_ref[:, block * LANES : (block + 1) * LANES] = jnp.concatenate(parts, axis=0).astype(BF16)


def parts_of(vector):
    real, imag = vector
    real_high, real_low = split(real)
    imag_high, imag_low = split(imag)
    return [real_high, imag_high, real_low, imag_low]


def precondition(vector, high_ref, low_ref, wide_ref):
    tiles = vector[0].shape[0]
    straight = parts_of(vector)
    turned = [-straight[1], straight[0], -straight[3], straight[2]]
    row = iota(vector[0].shape, 0)
    for tile in range(tiles):
        mask = row == tile
        put(wide_ref, 2 * tile, [jnp.where(mask, x, 0.0) for x in straight])
        put(wide_ref, 2 * tile + 1, [jnp.where(mask, x, 0.0) for x in turned])
    return product(high_ref, low_ref, wide_ref, 2 * tiles)


def load(ref):
    rows = ref.shape[0] // 2
    return ref[:rows], ref[rows:]


def save(ref, vector):
    ref[...] = jnp.concatenate(vector, axis=0)


def send(vector, first_ref, second_ref):
    even = lax.rem(lax.axis_index("dom"), 2) == 0
    rows = vector[0].shape[0]
    head = jnp.concatenate([vector[0][:1], vector[1][:1]], axis=0)
    tail = jnp.concatenate([vector[0][rows - 1 :], vector[1][rows - 1 :]], axis=0)
    first_ref[...] = jnp.where(even, tail, head)
    second_ref[...] = jnp.where(even, head, tail)


def mix_basis(coef, basis_ref):
    real, imag = coef
    tiles = basis_ref.shape[2] // LANES
    row = iota((tiles, LANES), 0)
    out_real = jnp.zeros((tiles, LANES), F32)
    out_imag = jnp.zeros((tiles, LANES), F32)
    for tile in range(tiles):
        lanes = slice(tile * LANES, (tile + 1) * LANES)
        base_real, base_imag = basis_ref[0, :, lanes], basis_ref[1, :, lanes]
        sum_real = jnp.sum(real * base_real - imag * base_imag, axis=0, keepdims=True)
        sum_imag = jnp.sum(real * base_imag + imag * base_real, axis=0, keepdims=True)
        out_real = jnp.where(row == tile, sum_real, out_real)
        out_imag = jnp.where(row == tile, sum_imag, out_imag)
    return out_real, out_imag


def coefficients(step, compact_ref, weights_ref, fresh_ref):
    beta = weights_ref[step]
    beta_real, beta_imag = beta[0:1], beta[1:2]
    compact_real, compact_imag = compact_ref[0], compact_ref[1]
    coef_real = jnp.sum(compact_real * beta_real - compact_imag * beta_imag, axis=1, keepdims=True)
    coef_imag = jnp.sum(compact_imag * beta_real + compact_real * beta_imag, axis=1, keepdims=True)
    fresh = fresh_ref[...]
    gamma_real = jnp.sum(beta_real * fresh[0:1] - beta_imag * fresh[1:2], axis=1, keepdims=True)
    gamma_imag = jnp.sum(beta_real * fresh[1:2] + beta_imag * fresh[0:1], axis=1, keepdims=True)
    return (coef_real, coef_imag), (gamma_real, gamma_imag)


def start_kernel(*refs):
    sources, refs = refs[:COPIED], refs[COPIED:]
    precond_in, refs = refs[0], refs[1:]
    right_ref, image_ref, first_ref, second_ref, high_ref, low_ref = refs[:6]
    targets, refs = refs[6 : 6 + COPIED], refs[6 + COPIED :]
    wide_ref, precond_ref, small_sem, tile_sem = refs
    moves = [
        pltpu.make_async_copy(source, target, small_sem.at[index])
        for index, (source, target) in enumerate(zip(sources, targets))
    ]
    tiles = precond_in.shape[0]
    tile_moves = [
        pltpu.make_async_copy(precond_in.at[tile], precond_ref.at[tile], tile_sem.at[tile])
        for tile in range(tiles)
    ]
    early, late = moves[:4], moves[4:]
    for move in early + tile_moves + late:
        move.start()
    for move in early:
        move.wait()
    basis_ref, compact_ref, weights_ref, fresh_ref = targets[:4]
    coef, _ = coefficients(0, compact_ref, weights_ref, fresh_ref)
    right = mix_basis(coef, basis_ref)
    save(right_ref, right)
    for tile in range(tiles):
        tile_moves[tile].wait()
        for part in range(2):
            store_parts(high_ref, low_ref, 2 * tile + part, precond_ref[tile, part])
    image = precondition(right, high_ref, low_ref, wide_ref)
    save(image_ref, image)
    send(image, first_ref, second_ref)
    for move in late:
        move.wait()


def as_column(row):
    count = row.shape[1]
    same = iota((count, count), 0) == iota((count, count), 1)
    return jnp.sum(jnp.where(same, row, 0.0), axis=1, keepdims=True)


def prepare_kernel(
    n_dom, count_ref, pattern_ref, rows_ref, side_ref, shifts_ref, mass_ref, k_ref, c_ref,
    high_ref, low_ref, c_high_ref, c_low_ref, pick_ref, below_ref, above_ref, drag_ref,
):
    tiles, slots_k, slots = k_ref.shape[0], k_ref.shape[1], c_ref.shape[0]
    for tile in range(tiles):
        for slot in range(slots_k):
            store_parts(high_ref, low_ref, tile * slots_k + slot, k_ref[tile, slot])
    for slot in range(slots):
        store_parts(c_high_ref, c_low_ref, slot, c_ref[slot])
    mine = lax.axis_index("sub") * tiles
    lane = iota((tiles, pick_ref.shape[1]), 1) ^ mine
    lane = lane.astype(F32)
    picked = [
        jnp.where(as_column(pattern_ref[slot : slot + 1].astype(F32)) == lane, 1.0, 0.0)
        for slot in range(slots_k - 1)
    ]
    pick_ref[...] = jnp.concatenate(picked, axis=0).astype(BF16)
    domain = lax.axis_index("dom")
    shape = (tiles, LANES)
    row = iota(shape, 0)
    for slot in range(slots):
        live = slot < count_ref[0]
        side = jnp.broadcast_to(side_ref[:, slot : slot + 1], shape)
        here = row == jnp.broadcast_to(rows_ref[:, slot : slot + 1], shape)
        low_on = jnp.where(live & (domain > 0), 1.0, 0.0)
        high_on = jnp.where(live & (domain < n_dom - 1), 1.0, 0.0)
        below_ref[slot] = jnp.where(here & (side == 0), low_on, 0.0)
        above_ref[slot] = jnp.where(here & (side != 0), high_on, 0.0)
    mass = mass_ref[...]
    for step in range(drag_ref.shape[0]):
        for part in range(2):
            shift = jnp.broadcast_to(shifts_ref[step : step + 1, part : part + 1], shape)
            drag_ref[step, part] = mass * shift


def inner_kernel(basis_ref, after_ref, inner_ref):
    real, imag = basis_ref[0], basis_ref[1]
    inner = nt_dot(real, jnp.concatenate([real, imag], axis=0), HIGH)
    inner = inner + nt_dot(imag, jnp.concatenate([imag, -real], axis=0), HIGH)
    half = inner_ref.shape[0]
    row, lane = iota((half, half), 0), iota((half, half), 1)

    def block(left, right, part):
        lanes = (2 * part + right) * half
        return inner[left * half : (left + 1) * half, lanes : lanes + half]

    low_real = block(1, 1, 0)
    pieces = [
        jnp.where(lane >= row, block(0, 0, 0), low_real),
        jnp.where(lane > row, block(0, 0, 1), jnp.where(lane < row, block(1, 1, 1), low_real)),
        block(0, 1, 0),
        block(0, 1, 1),
    ]
    inner_ref[...] = jnp.zeros(inner_ref.shape, F32)
    for index, piece in enumerate(pieces):
        inner_ref[:, (4 + index) * half : (5 + index) * half] = piece


def stiff_kernel(step, others, image_ref, *refs):
    blocks, (drag_ref, high_ref, low_ref, pick_ref) = refs[:others], refs[others : others + 4]
    result_ref, wide_ref = refs[-2:]
    image = load(image_ref)
    tiles = image[0].shape[0]
    own = parts_of(image)
    gathered = [own] + [parts_of(load(block)) for block in blocks]
    table = jnp.concatenate(
        [jnp.concatenate([g[part] for g in gathered], axis=0) for part in range(4)], axis=1
    ).astype(BF16)
    chosen = jnp.dot(pick_ref[...], table, preferred_element_type=F32)
    others = chosen.shape[0] // tiles
    row = iota(image[0].shape, 0)
    for tile in range(tiles):
        mask = row == tile
        base = tile * (others + 1)
        put(wide_ref, base, [jnp.where(mask, x, 0.0) for x in own])
        for slot in range(others):
            rows = slice(slot * tiles, (slot + 1) * tiles)
            put(
                wide_ref,
                base + 1 + slot,
                [
                    jnp.where(mask, chosen[rows, part * LANES : (part + 1) * LANES], 0.0)
                    for part in range(4)
                ],
            )
    stiff = product(high_ref, low_ref, wide_ref, tiles * (others + 1))
    drag = cmul((drag_ref[step, 0], drag_ref[step, 1]), image)
    save(result_ref, csub(stiff, drag))


def couple(partial_ref, first_ref, second_ref, high_ref, low_ref, below_ref, above_ref, wide_ref):
    even = lax.rem(lax.axis_index("dom"), 2) == 0
    first, second = first_ref[...], second_ref[...]
    below = jnp.where(even, second, first)
    above = jnp.where(even, first, second)
    below = parts_of((below[0:1], below[1:2]))
    above = parts_of((above[0:1], above[1:2]))
    slots = below_ref.shape[0]
    for slot in range(slots):
        low_mask, high_mask = below_ref[slot], above_ref[slot]
        put(wide_ref, slot, [low_mask * below[part] + high_mask * above[part] for part in range(4)])
    return cadd(load(partial_ref), product(high_ref, low_ref, wide_ref, slots))


def level_kernel(
    partial_ref, first_in, second_in, c_high, c_low, below_ref, above_ref, term_ref, p_high, p_low,
    result_ref, out_ref, first_ref, second_ref, *refs,
):
    next_refs, wide_ref = refs[:-1], refs[-1]
    result = couple(
        partial_ref, first_in, second_in, c_high, c_low, below_ref, above_ref, wide_ref
    )
    save(result_ref, result)
    term = csub(result, load(term_ref))
    for next_ref in next_refs:
        save(next_ref, term)
    image = precondition(term, p_high, p_low, wide_ref)
    save(out_ref, image)
    send(image, first_ref, second_ref)


def gram_kernel(basis_ref, previous_ref, inner_ref, *refs):
    refs, (out_ref, rows_ref) = refs[:-2], refs[-2:]
    results = [load(ref) for ref in refs[: ITERS - 1]]
    right = load(refs[ITERS - 1])
    images = [load(ref) for ref in refs[ITERS:]]
    zero = jnp.zeros(right[0].shape, F32)
    vectors = results + [(zero, zero), right] + images + [load(previous_ref)]
    count = len(vectors)
    for index, (real, imag) in enumerate(vectors):
        rows_ref[:, index, :] = real
        rows_ref[:, count + index, :] = imag
        rows_ref[:, 2 * count + index, :] = imag
        rows_ref[:, 3 * count + index, :] = -real
    tiles = rows_ref.shape[0]
    lefts, rights, chosen = [], [], []
    half = count // 2
    for tile in range(tiles):
        lanes = slice(tile * LANES, (tile + 1) * LANES)
        for part in range(2):
            left = rows_ref[tile, part * count : (part + 1) * count]
            lefts.append(jnp.concatenate([basis_ref[part, :, lanes], left], axis=0))
            base = 2 * part * count
            rights.append(rows_ref[tile, base : base + 2 * count])
            chosen.append(
                jnp.concatenate(
                    [
                        rows_ref[tile, base + half : base + count],
                        rows_ref[tile, base + count + half : base + 2 * count],
                    ],
                    axis=0,
                )
            )
    left = jnp.concatenate(lefts, axis=1)
    chosen = jnp.concatenate(chosen, axis=1)
    right_rows = jnp.concatenate([chosen, chosen, jnp.concatenate(rights, axis=1)], axis=0)
    table = nt_dot(left, right_rows, HIGH)
    width = table.shape[1]
    lane = iota((count, width), 1)
    merged = jnp.where(
        lane < count,
        table[:count],
        jnp.where(lane < 2 * count, table[count : 2 * count], table[2 * count :]),
    )
    out_ref[...] = jnp.concatenate([merged, inner_ref[:, width:]], axis=1)


def pack(total, fold):
    width = LANES // fold
    row, lane = iota(total.shape, 0), iota(total.shape, 1)
    kept = jnp.where(lane < width, total, 0.0)
    moved = kept
    for k in range(1, fold):
        moved = jnp.where(row % fold == k, pltpu.roll(kept, k * width, 1), moved)
    return jnp.concatenate(
        [
            jnp.sum(moved[k : k + fold], axis=0, keepdims=True)
            for k in range(0, total.shape[0], fold)
        ],
        axis=0,
    )


def unpack(packed, fold):
    width = LANES // fold
    rows = packed.shape[0]
    spread = jnp.concatenate(
        [jnp.broadcast_to(packed[k : k + 1], (fold, LANES)) for k in range(rows)], axis=0
    )
    row, lane = iota(spread.shape, 0), iota(spread.shape, 1)
    moved = spread
    for k in range(1, fold):
        moved = jnp.where(row % fold == k, pltpu.roll(spread, LANES - k * width, 1), moved)
    return jnp.where(lane < width, moved, 0.0)


def last_kernel(
    fold, partial_ref, first_in, second_in, c_high, c_low, below_ref, above_ref, sums_ref, *refs
):
    earlier, (payload_ref, wide_ref) = refs[:-2], refs[-2:]
    result = couple(
        partial_ref, first_in, second_in, c_high, c_low, below_ref, above_ref, wide_ref
    )
    vectors = [load(ref) for ref in earlier[: ITERS - 1]]
    total = sums_ref[...]
    count = total.shape[0]
    row, lane = iota(total.shape, 0), iota(total.shape, 1)
    base = 2 * count
    last = ITERS - 1
    pairs = [(index, last, vector, result) for index, vector in enumerate(vectors)]
    pairs += [(last, last, result, result), (last, ITERS, result, load(earlier[last]))]
    for at_row, at_col, left, right in pairs:
        real = left[0] * right[0] + left[1] * right[1]
        imag = left[0] * right[1] - left[1] * right[0]
        for part, value in enumerate((real, imag)):
            value = jnp.sum(jnp.sum(value, axis=0, keepdims=True), axis=1, keepdims=True)
            spot = (row == at_row) & (lane == base + part * count + at_col)
            total = jnp.where(spot, value, total)
    total = pack(total, fold)

    @pl.loop(0, payload_ref.shape[0])
    def _(device):
        payload_ref[device] = total


def settle(
    total_rows, sums, inner, basis_ref, images, previous,
):
    count = sums.shape[0]
    half = count // 2
    shape = sums.shape

    def column(lane, table=sums):
        return jnp.broadcast_to(table[:, lane : lane + 1], shape)

    def cell(row, lane):
        return jnp.broadcast_to(column(lane)[row : row + 1], shape)

    def entry(row, col):
        base = 2 * count
        return cell(row, base + col), cell(row, base + count + col)

    gram = {(a, b): entry(a, b) for a in range(ITERS) for b in range(a, ITERS)}
    target = [entry(a, ITERS) for a in range(ITERS)]
    lower, pivots = {}, []
    for col in range(ITERS):
        pivot = gram[col, col][0]
        for mid in range(col):
            real, imag = lower[col, mid]
            pivot = pivot - (real * real + imag * imag) * pivots[mid]
        pivots.append(pivot)
        for row in range(col + 1, ITERS):
            value = conj(gram[col, row])
            for mid in range(col):
                value = csub(value, scale(cmul(lower[row, mid], conj(lower[col, mid])), pivots[mid]))
            lower[row, col] = (value[0] / pivot, value[1] / pivot)
    forward = []
    for row in range(ITERS):
        value = target[row]
        for mid in range(row):
            value = csub(value, cmul(lower[row, mid], forward[mid]))
        forward.append(value)
    solved = [None] * ITERS
    for row in reversed(range(ITERS)):
        value = (forward[row][0] / pivots[row], forward[row][1] / pivots[row])
        for mid in range(row + 1, ITERS):
            value = csub(value, cmul(conj(lower[mid, row]), solved[mid]))
        solved[row] = value

    offset = ITERS + 1
    square = jnp.zeros(shape, F32)
    for a in range(ITERS):
        square = square + (solved[a][0] ** 2 + solved[a][1] ** 2) * entry(offset + a, offset + a)[0]
        for b in range(a + 1, ITERS):
            pair = cmul(conj(solved[a]), solved[b])
            square = square + 2.0 * cmul(pair, entry(offset + a, offset + b))[0]

    projections = []
    for block in range(2):
        base = block * count
        value = None
        for a in range(ITERS):
            term = cmul(solved[a], (column(base + a), column(base + half + a)))
            value = term if value is None else cadd(value, term)
        projections.append(scale(value, 1.0 / total_rows))
    value = None
    for a in range(ITERS):
        term = cmul(solved[a], entry(count - 1, offset + a))
        value = term if value is None else cadd(value, term)
    extra = scale(value, 1.0 / total_rows)

    row, lane = iota(shape, 0), iota(shape, 1)
    spot = lane - 4 * count
    column_of = spot % count
    zone = jnp.where((spot >= 0) & (spot < 4 * count), spot // count, 4)
    spread = [
        [
            jnp.sum(jnp.where(column_of == row, part, 0.0), axis=0, keepdims=True)
            for part in projections[block]
        ]
        for block in range(2)
    ]

    def real_weight(left, right):
        return left[0] * right[0] + left[1] * right[1]

    def imag_weight(left, right):
        return left[1] * right[0] - left[0] * right[1]

    first, second = projections
    same = real_weight(second, spread[1])
    upper, lower = column_of > row, column_of < row
    zones = [
        jnp.where(
            lower,
            2.0 * same,
            jnp.where(upper, 2.0, 1.0) * real_weight(first, spread[0]),
        ),
        jnp.where(
            upper,
            2.0 * imag_weight(first, spread[0]),
            jnp.where(lower, 2.0 * imag_weight(second, spread[1]), same),
        ),
        2.0 * real_weight(first, spread[1]),
        2.0 * imag_weight(first, spread[1]),
    ]
    weight = jnp.zeros(shape, F32)
    for index, value in enumerate(zones):
        weight = jnp.where(zone == index, value, weight)
    quad = jnp.sum(inner * weight, axis=1, keepdims=True)
    quad = jnp.broadcast_to(quad, shape)
    for block in range(2):
        base = block * count
        real, imag = projections[block]
        cross = cmul(
            cmul((real, -imag), extra), (column(base + half - 1), column(base + count - 1))
        )[0]
        quad = quad + 2.0 * cross - 2.0 * total_rows * (real * real + imag * imag)
    quad = jnp.broadcast_to(jnp.sum(quad, axis=0, keepdims=True), shape)
    extra_size = extra[0] * extra[0] + extra[1] * extra[1]
    quad = quad + extra_size * (entry(count - 1, count - 1)[0] - 2.0 * total_rows)
    norm = jnp.sqrt((square + quad) * (1.0 / total_rows) + EPSILON)

    coef = tuple(
        jnp.concatenate([projections[0][part], projections[1][part]], axis=0) for part in range(2)
    )
    mixed = cadd(mix_basis(coef, basis_ref), cmul(extra, previous))
    made = None
    for a in range(ITERS):
        term = cmul(solved[a], images[a])
        made = term if made is None else cadd(made, term)
    remain = csub(made, mixed)
    latest = (remain[0] / norm, remain[1] / norm)

    rows = []
    for part in range(2):
        spread = jnp.zeros(shape, F32)
        for block in range(2):
            spread = spread + jnp.where(lane == block * count + row, projections[block][part], 0.0)
        spread = jnp.sum(spread, axis=0, keepdims=True)
        spread = spread + jnp.where(lane[:1] == 2 * count, extra[part][:1], 0.0)
        if part == 0:
            spread = spread + jnp.where(lane[:1] == 2 * count + 1, norm[:1], 0.0)
        rows.append(spread)
    return latest, jnp.concatenate(rows, axis=0)


def reduce_sums(sums_ref):
    if sums_ref.shape[0] <= 64:
        values = [sums_ref[k] for k in range(sums_ref.shape[0])]
        while len(values) > 1:
            values = [
                values[k] + values[k + 1] if k + 1 < len(values) else values[k]
                for k in range(0, len(values), 2)
            ]
        return values[0]
    return jnp.sum(sums_ref[...], axis=0)


def between_kernel(
    total_rows, step, sums_ref, basis_ref, compact_ref, weights_ref, fresh_ref, p_high, p_low,
    *refs,
):
    images = [load(ref) for ref in refs[:ITERS]]
    previous_ref = refs[ITERS]
    (right_ref, image_ref, first_ref, second_ref, latest_ref, coeffs_ref, inner_ref, wide_ref) = refs[
        ITERS + 1 :
    ]
    sums = unpack(reduce_sums(sums_ref), FOLDS[step])
    inner_ref[...] = sums
    latest, coeffs = settle(total_rows, sums, sums, basis_ref, images, load(previous_ref))
    save(latest_ref, latest)
    coeffs_ref[...] = coeffs
    coef, gamma = coefficients(step + 1, compact_ref, weights_ref, fresh_ref)
    right = cadd(mix_basis(coef, basis_ref), cmul(gamma, latest))
    save(right_ref, right)
    image = precondition(right, p_high, p_low, wide_ref)
    save(image_ref, image)
    send(image, first_ref, second_ref)


def finish_kernel(total_rows, sums_ref, inner_ref, basis_ref, *refs):
    images = [load(ref) for ref in refs[:ITERS]]
    previous_ref, before_ref, made_ref, listed_ref = refs[ITERS:]
    sums = unpack(reduce_sums(sums_ref), FOLDS[-1])
    previous = load(previous_ref)
    latest, coeffs = settle(total_rows, sums, inner_ref[...], basis_ref, images, previous)
    for step, vector in enumerate((previous, latest)):
        for part in range(2):
            for tile in range(vector[part].shape[0]):
                made_ref[step, part : part + 1, tile * LANES : (tile + 1) * LANES] = vector[part][
                    tile : tile + 1
                ]
    width = listed_ref.shape[2]
    listed_ref[0] = before_ref[:, :width]
    listed_ref[1] = coeffs[:, :width]


def vmem():
    return pl.BlockSpec(memory_space=pltpu.VMEM)


def hbm():
    return pl.BlockSpec(memory_space=pltpu.HBM)


def smem():
    return pl.BlockSpec(memory_space=pltpu.SMEM)


def in_hbm(*arrays):
    return tuple(pltpu.with_memory_space_constraint(array, pltpu.HBM) for array in arrays)


def call(kernel, out_shape, in_specs, scratch, args, flops=10**7):
    return pl.pallas_call(
        kernel,
        out_shape=out_shape,
        in_specs=in_specs,
        out_specs=jax.tree.map(lambda _: vmem(), out_shape),
        scratch_shapes=scratch,
        cost_estimate=pl.CostEstimate(flops=flops, bytes_accessed=10**6, transcendentals=0),
        compiler_params=pltpu.CompilerParams(vmem_limit_bytes=VMEM_LIMIT),
    )(*args)


def local(
    n_dom,
    n_sub,
    basis,
    compact,
    weights,
    fresh,
    shifts,
    k_tiles,
    pattern,
    mass,
    precond,
    c_tiles,
    c_rows,
    c_side,
    c_count,
):
    tiles, slots_k, tile = k_tiles.shape[0], k_tiles.shape[1], k_tiles.shape[2]
    slots = c_tiles.shape[0]
    devices = n_dom * n_sub
    total_rows = float(tiles * tile * devices)
    steps = weights.shape[0]
    vec = jax.ShapeDtypeStruct((2 * tiles, tile), F32)
    edge = jax.ShapeDtypeStruct((2, tile), F32)
    square = jax.ShapeDtypeStruct((tiles, tile), F32)
    k_blocks = tiles * slots_k
    p_blocks = 2 * tiles
    k_part = jax.ShapeDtypeStruct((tile, k_blocks * tile), BF16)
    c_part = jax.ShapeDtypeStruct((tile, slots * tile), BF16)
    p_part = jax.ShapeDtypeStruct((tile, p_blocks * tile), BF16)
    mask = jax.ShapeDtypeStruct((slots, tiles, tile), F32)
    pick = jax.ShapeDtypeStruct(((slots_k - 1) * tiles, tiles * n_sub), BF16)
    drag = jax.ShapeDtypeStruct((steps, 2, tiles, tile), F32)
    compact = jnp.swapaxes(compact, 1, 2)
    pattern = pattern.T
    mass = mass.reshape(tiles, tile)
    zero = jnp.zeros((2 * tiles, tile), F32)

    def wide(blocks):
        return pltpu.VMEM((4 * tiles, blocks * tile), BF16)

    even_swap = [(i, i ^ 1) for i in range(n_dom)]
    odd_swap = []
    for i in range(n_dom):
        other = i + 1 if i % 2 else i - 1
        for j in range(n_sub):
            inside = 0 <= other < n_dom
            target = other * n_sub + j if inside else i * n_sub + (j ^ 1)
            odd_swap.append((i * n_sub + j, target))

    def exchange(image, first, second):
        second = lax.ppermute(second, AXES, odd_swap)
        first = lax.ppermute(first, "dom", even_swap)
        blocks = []
        for k in range(1, n_sub):
            blocks.append(lax.ppermute(image, "sub", [(i, i ^ k) for i in range(n_sub)]))
        return blocks, first, second

    copied = (
        basis, compact, weights, fresh, pattern, c_rows.reshape(1, slots), c_side.reshape(1, slots),
        shifts, mass, c_tiles,
    )
    (right, image, first, second, p_high, p_low, *copied) = call(
        start_kernel,
        (vec, vec, edge, edge, p_part, p_part)
        + tuple(pltpu.VMEM(array.shape, array.dtype) for array in copied),
        [hbm()] * (len(copied) + 1),
        [
            wide(p_blocks),
            pltpu.VMEM(precond.shape, F32),
            pltpu.SemaphoreType.DMA((len(copied),)),
            pltpu.SemaphoreType.DMA((tiles,)),
        ],
        in_hbm(*copied, precond),
    )
    basis, compact, weights, fresh = copied[:4]
    k_high, k_low, c_high, c_low, pick_table, below, above, drag = call(
        functools.partial(prepare_kernel, n_dom),
        (k_part, k_part, c_part, c_part, pick, mask, mask, drag),
        [smem()] + [vmem()] * 7, [], (c_count, *copied[4:9], k_tiles, copied[9]),
    )
    previous = zero
    for step in range(steps):
        term = right
        images, results = [image], []
        for index in range(ITERS):
            blocks, first_in, second_in = exchange(image, first, second)
            ahead = ()
            if step == 0 and index == ITERS - 2:
                inner = call(inner_kernel, square, [vmem()] * 2, [], (basis, image))
                ahead = (inner,)
            partial = call(
                functools.partial(stiff_kernel, step, n_sub - 1), vec,
                [vmem()] * (n_sub + 4 + len(ahead)), [wide(k_blocks)],
                (image, *blocks, drag, k_high, k_low, pick_table, *ahead),
            )
            common = (partial, first_in, second_in, c_high, c_low, below, above)
            if index + 1 < ITERS:
                later = [vec] if index + 2 < ITERS else []
                result, image, first, second, *later = call(
                    level_kernel, (vec, vec, edge, edge, *later), [vmem()] * 10,
                    [wide(max(slots, p_blocks))], common + (term, p_high, p_low),
                )
                term = later[0] if later else None
                results.append(result)
                images.append(image)
            else:
                sums = call(
                    gram_kernel, square, [vmem()] * (3 + 2 * ITERS),
                    [pltpu.VMEM((tiles, 4 * tiles, tile), F32)],
                    (basis, previous, inner, *results, right, *images),
                )
                fold = FOLDS[step]
                payload = call(
                    functools.partial(last_kernel, fold),
                    jax.ShapeDtypeStruct((devices, tiles // fold, tile), F32),
                    [vmem()] * (8 + ITERS), [wide(slots)], common + (sums, *results, right),
                )
        sums = lax.all_to_all(payload, AXES, 0, 0)
        if step + 1 < steps:
            right, image, first, second, latest, coeffs, inner_sum = call(
                functools.partial(between_kernel, total_rows, step),
                (vec, vec, edge, edge, vec, jax.ShapeDtypeStruct((2, tile), F32), square),
                [vmem()] * (8 + ITERS), [wide(p_blocks)],
                (sums, basis, compact, weights, fresh, p_high, p_low, *images, previous),
            )
            previous = latest
        else:
            width = basis.shape[1] + 2
            made, listed = call(
                functools.partial(finish_kernel, total_rows),
                (
                    jax.ShapeDtypeStruct((steps, 2, tiles * tile), F32),
                    jax.ShapeDtypeStruct((steps, 2, width), F32),
                ),
                [vmem()] * (5 + ITERS), [],
                (sums, inner_sum, basis, *images, previous, coeffs),
            )
    return made, listed


def solution(mesh):
    placed = (
        P(None, None, AXES),
        P(),
        P(),
        P(),
        P(),
        P(AXES, None, None, None),
        P(AXES, None),
        P(AXES),
        P(AXES, None, None, None),
        P(AXES, None, None),
        P(AXES),
        P(AXES),
        P(AXES),
    )
    return jax.shard_map(
        functools.partial(local, mesh.shape["dom"], mesh.shape["sub"]),
        mesh=mesh,
        in_specs=placed,
        out_specs=(P(None, None, AXES), P()),
        check_vma=False,
    )
```
